128 devices in a mesh: groups: 4 (over y, x), seq: 16 (over z), sub: 2 (over core).
Axes of the slice: x: 2, y: 2, z: 16, core: 2. Of those that a mesh axis runs over, the one named last changes fastest.
The devices are a block of a 8x8x16 slice.
Arguments:
- query_proj: bfloat16 [8192, 4096], P(('groups', 'seq'), 'sub'), parts along dimension 0, may hold values from -2500 to 2500
- key_proj: bfloat16 [8192, 4096], P(('groups', 'seq'), 'sub'), parts along dimension 0, may hold values from -2500 to 2500
- value_proj: bfloat16 [8192, 4096], P(('groups', 'seq'), 'sub'), parts along dimension 0, may hold values from -12 to 12
- out_weight: bfloat16 [4096, 5120], P('sub', 'seq'), may hold values from -0.5 to 0.5
- query_gain: float32 [4096], P('sub'), may hold values from 0.25 to 1.75
- key_gain: float32 [4096], P('sub'), may hold values from 0.25 to 1.75
- gate_scale: float32 [20480], P(('groups', 'sub')), parts along dimension 0, may hold values from 0.5 to 2
- key_count: int32 [4], P('groups'), parts along dimension 0, may hold values from 1024 to 2048
Outputs:
- attended_out: bfloat16 [8192, 5120], P(('groups', 'seq'), 'sub'), parts along dimension 0
The draws below stay inside these ranges and needn't reach their ends.
There are 4 independent parts, one for each index of `groups`. The reference program is written for one: setup_inputs(seed, part) draws one part's arguments, and reference() takes and returns one part's arrays. A program takes and returns all parts, laid end to end along the dimension named above; an argument that names none is the same for every part. Nothing has to cross between parts.
All inputs are finite; a program needn't handle non-finite values.
Results may differ from the reference program's by a relative error of at most 0.012.
Values may be sent and summed in bfloat16 or wider, within the bound.
A program may use at most 128 MiB of HBM per device.

```python
import math
import jax
import jax.numpy as jnp
from jax import lax

D = 5120
HD = 128
HEADS = 32
SEQ = 2048


def queries_keys(key):
    folded = jax.random.fold_in(key, 4711)
    streams = jax.random.split(folded, 6)
    features = HEADS * HD
    head_ramp = 3.0 ** ((jnp.arange(features) // HD).astype(jnp.float32) / max(HEADS - 1, 1))
    column_query = jnp.exp(jax.random.uniform(streams[0], (features,), minval=0.0, maxval=math.log(10.0))) * head_ramp
    column_key = jnp.exp(jax.random.uniform(streams[1], (features,), minval=0.0, maxval=math.log(10.0))) * head_ramp
    rows_query = jnp.exp(jax.random.uniform(streams[2], (SEQ, 1), minval=0.0, maxval=math.log(10.0)))
    rows_key = jnp.exp(jax.random.uniform(streams[3], (SEQ, 1), minval=0.0, maxval=math.log(10.0)))
    noise_query = jnp.clip(jax.random.normal(streams[4], (SEQ, features)), -4.0, 4.0)
    noise_key = jnp.clip(jax.random.normal(streams[5], (SEQ, features)), -4.0, 4.0)
    query_draw = noise_query * column_query * rows_query
    key_draw = noise_key * column_key * rows_key
    return (query_draw, key_draw)


def draw_query_proj(key, part):
    return queries_keys(key)[0].astype(jnp.bfloat16)


def draw_key_proj(key, part):
    return queries_keys(key)[1].astype(jnp.bfloat16)


def block_levels(own_key, shape, cuts, low, top_value):
    def one(dim, parts):
        draws = jax.random.uniform(jax.random.fold_in(jax.random.fold_in(own_key, 6), dim), (parts,), jnp.float32, low / len(cuts), top_value / len(cuts))
        return jnp.repeat(jnp.exp(draws), shape[dim] // parts).reshape((-1,) + (1,) * (len(shape) - dim - 1))

    level = one(*cuts[0])
    for cut in cuts[1:]:
        level = level * one(*cut)
    return level


def scatter_about(key, extent, deviation, most, cuts=(), kind=jnp.bfloat16):
    entries = jax.random.normal(key, extent, jnp.float32) * deviation
    if len(cuts) > 0:
        entries = block_levels(key, extent, cuts, -0.22, 0.18) * entries
    return jnp.clip(entries, min=-most, max=most).astype(kind)


def setup_inputs(seed: int = 0, part: int = 0) -> dict:
    key_of = jax.random.split(jax.random.key(seed), 9)
    own_keys = jax.random.split(jax.random.fold_in(key_of[8], part), 9)
    return {
        "query_proj": draw_query_proj(jax.random.fold_in(jax.random.fold_in(key_of[8], part), 71), part),
        "key_proj": draw_key_proj(jax.random.fold_in(jax.random.fold_in(key_of[8], part), 71), part),
        "value_proj": scatter_about(own_keys[2], (SEQ, HEADS * HD), 2.0, 12.0, ((0, 16), (1, 2))),
        "out_weight": scatter_about(key_of[3], (HEADS * HD, D), HD ** -0.5, 0.5, ((0, 2), (1, 16))),
        "query_gain": jnp.clip(1.0 + 0.15 * jax.random.normal(key_of[4], (HEADS * HD,), jnp.float32), 0.25, 1.75),
        "key_gain": jnp.clip(1.0 + 0.15 * jax.random.normal(key_of[5], (HEADS * HD,), jnp.float32), 0.25, 1.75),
        "gate_scale": jnp.clip(jnp.exp(math.log(2.0) - 1.3862944 * jax.random.uniform(own_keys[6], (D,), jnp.float32) ** block_levels(own_keys[6], (D,), ((0, 2),), -0.2, 0.2)), 0.5, 2.0),
        "key_count": jax.random.randint(own_keys[7], (1,), SEQ // 2, SEQ + 1).astype(jnp.int32),
    }


epsilon = 1e-06

def rms_scaled(inputs, gain):
    wide = inputs.astype(jnp.float32)
    return wide * lax.rsqrt(lax.optimization_barrier(jnp.mean(wide * wide, axis=-1, keepdims=True)) + epsilon) * gain

def reference(query_proj, key_proj, value_proj, out_weight, query_gain, key_gain, gate_scale, key_count):
    query_normed = rms_scaled(query_proj, query_gain).astype(jnp.bfloat16)
    key_normed = rms_scaled(key_proj, key_gain).astype(jnp.bfloat16)
    usable = jnp.arange(SEQ) < key_count[0]
    scale = 1.0 / HD ** 0.5
    query_heads = query_normed.reshape(SEQ, HEADS, HD).transpose(1, 0, 2)
    key_heads = key_normed.reshape(SEQ, HEADS, HD).transpose(1, 0, 2)
    value_heads = value_proj.reshape(SEQ, HEADS, HD).transpose(1, 0, 2)

    def one_head(operands):
        query_head, key_head, value_head = operands
        scores = jnp.dot(query_head, key_head.T, preferred_element_type=jnp.float32) * scale
        scores = jnp.where(usable[None, :], scores, -1e+30)
        highest = lax.optimization_barrier(jnp.max(scores, axis=1, keepdims=True))
        weights = jnp.where(usable[None, :], jnp.exp(scores - highest), 0.0)
        denominator = lax.optimization_barrier(jnp.sum(weights, axis=1, keepdims=True))
        summed = jnp.dot(weights.astype(jnp.bfloat16), value_head, preferred_element_type=jnp.float32)
        return (summed / denominator).astype(jnp.bfloat16)
    results = lax.map(one_head, (query_heads, key_heads, value_heads))
    attended = results.transpose(1, 0, 2).reshape(SEQ, HEADS * HD)
    projected = jnp.dot(attended, out_weight, preferred_element_type=jnp.float32)
    return (projected * gate_scale).astype(jnp.bfloat16)
```

```python
import functools
import math

import jax
import jax.numpy as jnp
from jax import lax
from jax.experimental import pallas as pl
from jax.experimental.pallas import tpu as pltpu
from jax.sharding import PartitionSpec as P

HD = 128
EPSILON = 1e-06
MEMBERS = 4
CHUNK = 32
EARLY = 4
EVERY = 2
F32, BF16 = jnp.float32, jnp.bfloat16


def remote(source, target, send, arrive, where):
    return pltpu.make_async_remote_copy(
        src_ref=source,
        dst_ref=target,
        send_sem=send,
        recv_sem=arrive,
        device_id=where,
        device_id_type=pl.DeviceIdType.MESH,
    )


def nt(left, right):
    return lax.dot_general(left, right, (((1,), (1,)), ((), ())), preferred_element_type=F32)


def kernel(
    n, side, subs,
    q_in, k_in, v_in, w_in, q_gain, k_gain, gate_in, count,
    out,
    squares, squares_in, kn, qn, k_all, v_all, q_all, bias, o_out,
    att, w_half, w_all, gates, result,
    v_send, v_recv, k_send, k_recv, q_send, q_recv, o_send, o_recv,
    w_up, w_down, w_recv, small_send, small_recv, gate_send, gate_recv,
    att_send, att_recv, pair_send, pair_recv, out_send, out_recv,
):
    tokens, features = q_in.shape
    width = w_in.shape[1]
    planes = n // (MEMBERS * subs)
    columns = planes * width
    z = lax.axis_index("seq")
    s = lax.axis_index("sub")
    g = lax.axis_index("groups")
    gx, gy = g % side, g // side
    bx, by = gx % 2, gy % 2
    me = 2 * by + bx

    def square(e):
        there = g + (e % 2) * (1 - 2 * bx) + (e // 2) * side * (1 - 2 * by)
        return there, 2 * ((by + e // 2) % 2) + (bx + e) % 2

    def hop(i):
        return (i % 2) * ((i + 1) // 2) + (1 - i % 2) * ((n - i // 2) % n)

    barrier = pltpu.get_barrier_semaphore()

    def greet(i, carry):
        pl.semaphore_signal(barrier, inc=1, device_id={"seq": (z + i) % n}, device_id_type=pl.DeviceIdType.MESH)
        return carry

    lax.fori_loop(1, n, greet, 0)
    pl.semaphore_signal(barrier, inc=1, device_id={"sub": 1 - s}, device_id_type=pl.DeviceIdType.MESH)
    for e in range(1, MEMBERS):
        pl.semaphore_signal(barrier, inc=1, device_id={"groups": square(e)[0]}, device_id_type=pl.DeviceIdType.MESH)

    for index, array in enumerate((k_in, q_in)):
        total = jnp.zeros((tokens, HD), F32)
        for head in range(features // HD):
            wide = array[:, head * HD : (head + 1) * HD].astype(F32)
            total = total + wide * wide
        squares[index] = total

    pl.semaphore_wait(barrier, n - 1 + 1 + MEMBERS - 1)

    def to_peers(source, target, send, arrive):
        def one(i, carry):
            d = hop(i)
            there = (z + d) % n
            remote(source(there), target.at[pl.ds(pl.multiple_of(z * tokens, tokens), tokens), :],
                   send.at[d], arrive.at[d], {"seq": there}).start()
            return carry

        lax.fori_loop(1, n, one, 0)

    pair = remote(squares, squares_in, small_send.at[0], small_recv.at[0], {"sub": 1 - s})
    pair.start()
    to_peers(lambda there: v_in.at[:, pl.ds(pl.multiple_of(there * HD, HD), HD)], v_all, v_send, v_recv)
    gate_copies = []
    for e in range(1, MEMBERS):
        there, number = square(e)
        gate_copies.append(remote(gate_in.at[number], gates.at[me], gate_send.at[e], gate_recv.at[e], {"groups": there}))
        gate_copies[-1].start()
    gates[me] = gate_in[me]

    own = pl.ds(pl.multiple_of(z * tokens, tokens), tokens)
    pair.wait()
    for index, (array, gain, normed, full, send, arrive) in enumerate(
        ((k_in, k_gain, kn, k_all, k_send, k_recv), (q_in, q_gain, qn, q_all, q_send, q_recv))
    ):
        total = jnp.sum(squares[index] + squares_in[index], axis=1, keepdims=True)
        inverse = lax.rsqrt(total / (features * subs) + EPSILON)
        for head in range(features // HD):
            here = slice(head * HD, (head + 1) * HD)
            normed[head] = (array[:, here].astype(F32) * inverse * gain[:, here]).astype(BF16)
        to_peers(lambda there, normed=normed: normed.at[there], full, send, arrive)
        full[own, :] = normed[z]
    v_all[own, :] = v_in[:, pl.ds(pl.multiple_of(z * HD, HD), HD)]
    positions = lax.broadcasted_iota(jnp.int32, bias.shape, 1)
    bias[...] = jnp.where(positions < count[0], 0.0, -1e30)

    per_half = n // subs
    half_of, place = z // per_half, z % per_half
    gives = me == place // planes
    piece_rows = pl.ds(pl.multiple_of((place % planes) * width, 16), width)
    my_half = pl.ds(pl.multiple_of(s * features, features), features)
    weight_copy = remote(w_half, w_all.at[piece_rows, my_half], small_send.at[1], small_recv.at[1], {"sub": 1 - s})

    @pl.when(gives)
    def _():
        for head in range(features // HD):
            here = slice(head * HD, (head + 1) * HD)
            w_half[:, here] = jnp.transpose(w_in[here, :])

        @pl.when(s != half_of)
        def _():
            weight_copy.start()

        @pl.when(s == half_of)
        def _():
            def move(i, carry):
                row = pl.multiple_of((place % planes) * width + i * 16, 16)
                w_all[pl.ds(row, 16), my_half] = w_half[pl.ds(pl.multiple_of(i * 16, 16), 16), :]
                return carry

            lax.fori_loop(0, width // 16, move, 0)
            weight_copy.wait_recv()

    pieces = width // CHUNK
    events = planes * pieces
    reach = n // 2 - 1

    def ring(e):
        plane = per_half * s + planes * me + e // pieces
        k = (z - plane + n) % n
        rows = w_all.at[pl.ds(pl.multiple_of(e * CHUNK, CHUNK), CHUNK), :]
        up = remote(rows, rows, w_up.at[e], w_recv.at[e], {"seq": (z + 1) % n})
        down = remote(rows, rows, w_down.at[e], w_recv.at[e], {"seq": (z + n - 1) % n})
        return k, k < reach, (k == 0) | (k >= reach + 2), up, down

    def relay(e):
        k, goes_up, goes_down, up, down = ring(e)

        @pl.when(k != 0)
        def _():
            up.wait_recv()

        @pl.when(goes_up)
        def _():
            up.start()

        @pl.when(goes_down)
        def _():
            down.start()

    def relay_some(first, last):
        def one(e, carry):
            relay(e)
            return carry

        lax.fori_loop(first, last, one, 0)

    relay_some(0, EARLY)

    def arrived(i, carry):
        d = hop(i)
        for full, send, arrive in ((v_all, v_send, v_recv), (k_all, k_send, k_recv)):
            there = full.at[own, :]
            remote(there, there, send.at[d], arrive.at[d], {"seq": z}).wait_recv()
        return carry

    lax.fori_loop(1, n, arrived, 0)
    factor = math.log2(math.e) / math.sqrt(HD)
    mine = pl.ds(pl.multiple_of((s * MEMBERS + me) * tokens, tokens), tokens)

    def o_copy(d):
        lanes = pl.ds(pl.multiple_of(z * HD, HD), HD)
        return remote(o_out.at[d], att.at[mine, lanes], o_send.at[d], o_recv.at[d], {"seq": (z - d + n) % n})

    def attend(i, carry):
        d = hop(i)
        rows = pl.ds(pl.multiple_of(((z - d + n) % n) * tokens, tokens), tokens)

        @pl.when(i > 0)
        def _():
            there = q_all.at[own, :]
            remote(there, there, q_send.at[d], q_recv.at[d], {"seq": z}).wait_recv()

        scores = nt(q_all[rows, :], k_all[...]) * factor + bias[0:1, :]
        weights = jnp.exp2(scores - jnp.max(scores, axis=1, keepdims=True))
        denominator = jnp.sum(weights, axis=1, keepdims=True)
        summed = jnp.dot(weights.astype(BF16), v_all[...], preferred_element_type=F32)
        o_out[d] = (summed / denominator).astype(BF16)

        @pl.when(i > 0)
        def _():
            o_copy(d).start()

        @pl.when(i % EVERY == EVERY - 1)
        def _():
            relay(EARLY + i // EVERY)

        return carry

    lax.fori_loop(0, n, attend, 0)
    att[mine, pl.ds(pl.multiple_of(z * HD, HD), HD)] = o_out[0]
    done = EARLY + n // EVERY

    def o_arrived(i, carry):
        o_copy(hop(i)).wait_recv()

        @pl.when((i % 2 == 0) & (done + i // 2 <= events))
        def _():
            relay(done + i // 2 - 1)

        return carry

    lax.fori_loop(1, n, o_arrived, 0)
    done = min(events, done + (n - 1) // 2)

    def block(half, number):
        return att.at[pl.ds(pl.multiple_of((half * MEMBERS + number) * tokens, tokens), tokens), :]

    square_copies, pair_copies = {}, {}
    for e in range(1, MEMBERS):
        square_copies[e] = remote(block(s, me), block(s, me), att_send.at[e], att_recv.at[e], {"groups": square(e)[0]})
        square_copies[e].start()
    for e in range(MEMBERS):
        number = square(e)[1]
        pair_copies[e] = remote(block(s, number), block(s, number), pair_send.at[e], pair_recv.at[e], {"sub": 1 - s})
        if e:
            square_copies[e].wait_recv()
        pair_copies[e].start()
    for e in range(MEMBERS):
        pair_copies[e].wait_recv()
    for copy in gate_copies:
        copy.wait_recv()

    starts = list(range(0, columns, 256))
    out_copies = []
    for index, first in enumerate(starts):
        last = min(columns, first + 256)
        needed = -(-last // CHUNK)
        if needed > done:
            relay_some(done, needed)
            done = needed
        total = nt(att[0 : MEMBERS * tokens, :], w_all[first:last, 0:features])
        for half in range(1, subs):
            total = total + nt(
                att[half * MEMBERS * tokens : (half + 1) * MEMBERS * tokens, :],
                w_all[first:last, half * features : (half + 1) * features],
            )
        for number in range(MEMBERS):
            scaled = total[number * tokens : (number + 1) * tokens, :] * gates[number][0:1, first:last]
            result[number, :, first:last] = scaled.astype(BF16)
        lanes = pl.ds(pl.multiple_of(me * columns + first, HD), last - first)
        for e in range(1, MEMBERS):
            there, number = square(e)
            copy = remote(result.at[number, :, pl.ds(first, last - first)], out.at[:, lanes],
                          out_send.at[index, e], out_recv.at[index, e], {"groups": there})
            copy.start()
            out_copies.append(copy)
        out[:, lanes] = result[me, :, first:last]

    def sent(i, carry):
        d = hop(i)
        there = k_all.at[own, :]
        for send, arrive in ((v_send, v_recv), (k_send, k_recv), (q_send, q_recv)):
            remote(there, there, send.at[d], arrive.at[d], {"seq": z}).wait_send()
        o_copy(d).wait_send()
        return carry

    lax.fori_loop(1, n, sent, 0)

    def relayed(e, carry):
        _, goes_up, goes_down, up, down = ring(e)

        @pl.when(goes_up)
        def _():
            up.wait_send()

        @pl.when(goes_down)
        def _():
            down.wait_send()

        return carry

    lax.fori_loop(0, events, relayed, 0)

    @pl.when(gives & (s != half_of))
    def _():
        weight_copy.wait_send()

    for copy in gate_copies + list(square_copies.values()) + list(pair_copies.values()):
        copy.wait_send()
    for copy in out_copies:
        copy.wait()


def shards(n, groups, subs, q, k, v, weight, q_gain, k_gain, gate, count):
    tokens, features = q.shape
    width = weight.shape[1]
    planes = n // (MEMBERS * subs)
    columns = planes * width
    events = planes * (width // CHUNK)
    blocks = -(-columns // 256)
    gate = jnp.broadcast_to(gate.reshape(MEMBERS, 1, columns), (MEMBERS, 8, columns))
    vmem = pl.BlockSpec(memory_space=pltpu.VMEM)
    dma = pltpu.SemaphoreType.DMA
    rows = n * tokens
    return pl.pallas_call(
        functools.partial(kernel, n, math.isqrt(groups), subs),
        out_shape=jax.ShapeDtypeStruct((tokens, MEMBERS * columns), BF16),
        in_specs=[vmem] * 7 + [pl.BlockSpec(memory_space=pltpu.SMEM)],
        out_specs=vmem,
        scratch_shapes=[
            pltpu.VMEM((2, tokens, HD), F32),
            pltpu.VMEM((2, tokens, HD), F32),
            pltpu.VMEM((n, tokens, HD), BF16),
            pltpu.VMEM((n, tokens, HD), BF16),
            pltpu.VMEM((rows, HD), BF16),
            pltpu.VMEM((rows, HD), BF16),
            pltpu.VMEM((rows, HD), BF16),
            pltpu.VMEM((8, rows), F32),
            pltpu.VMEM((n, tokens, HD), BF16),
            pltpu.VMEM((subs * MEMBERS * tokens, features), BF16),
            pltpu.VMEM((width, features), BF16),
            pltpu.VMEM((columns, subs * features), BF16),
            pltpu.VMEM((MEMBERS, 8, columns), F32),
            pltpu.VMEM((MEMBERS, tokens, columns), BF16),
        ]
        + [dma((n,))] * 8
        + [dma((events,))] * 3
        + [dma((2,))] * 2
        + [dma((MEMBERS,))] * 6
        + [dma((blocks, MEMBERS))] * 2,
        compiler_params=pltpu.CompilerParams(
            collective_id=0, has_side_effects=True, vmem_limit_bytes=56 * 2**20
        ),
        name="attention",
    )(q, k, v, weight, q_gain.reshape(1, -1), k_gain.reshape(1, -1), gate, count)


def solution(mesh):
    placed = (
        P(("groups", "seq"), "sub"),
        P(("groups", "seq"), "sub"),
        P(("groups", "seq"), "sub"),
        P("sub", "seq"),
        P("sub"),
        P("sub"),
        P(("groups", "sub")),
        P("groups"),
    )
    return jax.shard_map(
        functools.partial(shards, mesh.shape["seq"], mesh.shape["groups"], mesh.shape["sub"]),
        mesh=mesh,
        in_specs=placed,
        out_specs=P(("groups", "seq"), "sub"),
        check_vma=False,
    )
```

```python
import functools
import math

import jax
import jax.numpy as jnp
from jax import lax
from jax.experimental import pallas as pl
from jax.experimental.pallas import tpu as pltpu
from jax.sharding import PartitionSpec as P

HD = 128
EPSILON = 1e-06
MEMBERS = 4
CUTS = (48, 32)
IN_ATTENTION = ((12, 1), (16, 2))
IN_RETURN = ((6, 3), (12, 4))
IN_SQUARE = {0: 5, 2: 6}
IN_PROJECTION = ((5, 7), (13, 8))
F32, BF16 = jnp.float32, jnp.bfloat16


def remote(source, target, send, arrive, where):
    return pltpu.make_async_remote_copy(
        src_ref=source,
        dst_ref=target,
        send_sem=send,
        recv_sem=arrive,
        device_id=where,
        device_id_type=pl.DeviceIdType.MESH,
    )


def nt(left, right):
    return lax.dot_general(left, right, (((1,), (1,)), ((), ())), preferred_element_type=F32)


def kernel(
    n, side, subs,
    q_any, k_any, v_any, w_any, q_gain, k_gain, gate_in, count,
    out,
    q_in, k_in, v_in, gate_turned, squares, squares_in, kn, qn, k_all, v_all, q_all, bias, o_out,
    att, w_ring, w_pair, gates, result,
    load, v_send, v_recv, k_send, k_recv, q_send, q_recv, o_send, o_recv,
    ring_send, ring_recv, w_send, w_recv, small_send, small_recv, gate_send, gate_recv,
    att_send, att_recv, pair_send, pair_recv, out_send, out_recv,
):
    tokens, features = q_in.shape
    share = w_any.shape[0] // MEMBERS
    per_half = n // subs
    z = lax.axis_index("seq")
    s = lax.axis_index("sub")
    g = lax.axis_index("groups")
    gx, gy = g % side, g // side
    bx, by = gx % 2, gy % 2
    me = 2 * by + bx

    def square(e):
        there = g + (e % 2) * (1 - 2 * bx) + (e // 2) * side * (1 - 2 * by)
        return there, 2 * ((by + e // 2) % 2) + (bx + e) % 2

    def hop(i):
        return (i % 2) * ((i + 1) // 2) + (1 - i % 2) * ((n - i // 2) % n)

    barrier = pltpu.get_barrier_semaphore()

    def greet(i, carry):
        pl.semaphore_signal(barrier, inc=1, device_id={"seq": (z + i) % n}, device_id_type=pl.DeviceIdType.MESH)
        return carry

    lax.fori_loop(1, n, greet, 0)
    pl.semaphore_signal(barrier, inc=1, device_id={"sub": 1 - s}, device_id_type=pl.DeviceIdType.MESH)
    for e in range(1, MEMBERS):
        pl.semaphore_signal(barrier, inc=1, device_id={"groups": square(e)[0]}, device_id_type=pl.DeviceIdType.MESH)

    loads = [
        pltpu.make_async_copy(source, target, load.at[index])
        for index, (source, target) in enumerate(((k_any, k_in), (q_any, q_in), (v_any, v_in)))
    ]
    for copy in loads:
        copy.start()

    for index, array in enumerate((k_in, q_in)):
        loads[index].wait()
        total = jnp.zeros((tokens, HD), F32)
        for head in range(features // HD):
            wide = array[:, head * HD : (head + 1) * HD].astype(F32)
            total = total + wide * wide
        squares[index] = total

    weight_load = pltpu.make_async_copy(
        w_any.at[pl.ds(pl.multiple_of(me * share, 16), share), :],
        w_ring.at[pl.ds(pl.multiple_of(z * share, 16), share), :],
        load.at[3],
    )
    weight_load.start()

    gate = gate_in[...].reshape(1, gate_in.shape[0])
    for first in range(0, gate_in.shape[0], HD):
        gate_turned[first : first + HD, :] = jnp.transpose(jnp.broadcast_to(gate[:, first : first + HD], (HD, HD)))
    loads[2].wait()
    with jax.named_scope("barrier"):
        pl.semaphore_wait(barrier, n - 1 + 1 + MEMBERS - 1)

    pair = remote(squares, squares_in, small_send.at[0], small_recv.at[0], {"sub": 1 - s})
    pair.start()

    own = pl.ds(pl.multiple_of(z * tokens, tokens), tokens)

    def v_block(there):
        return v_in.at[:, pl.ds(pl.multiple_of(there * HD, HD), HD)]

    exchanges = (
        (v_block, v_all, v_send, v_recv),
        (lambda there: kn.at[there], k_all, k_send, k_recv),
        (lambda there: qn.at[there], q_all, q_send, q_recv),
    )

    def to_peers(array, first, last):
        source, target, send, arrive = exchanges[array]

        def one(i, carry):
            d = hop(i)
            there = (z + d) % n
            remote(source(there), target.at[own, :], send.at[d], arrive.at[d], {"seq": there}).start()
            return carry

        lax.fori_loop(first, last, one, 0)

    to_peers(0, 1, n)

    def gate_rows(i, number):
        return pl.ds(pl.multiple_of((i * MEMBERS + number) * share, 16), share)

    def gate_copy(i, e):
        there, number = square(e)
        return remote(gate_turned.at[gate_rows(i, number), :],
                      gates.at[pl.ds(pl.multiple_of((me * per_half + i) * share, 16), share), :],
                      gate_send.at[i, e], gate_recv.at[i, e], {"groups": there})

    def gate_out(i, carry):
        for e in range(1, MEMBERS):
            gate_copy(i, e).start()
        gates[pl.ds(pl.multiple_of((me * per_half + i) * share, 16), share), :] = gate_turned[gate_rows(i, me), :]
        return carry

    lax.fori_loop(0, per_half, gate_out, 0)

    pair.wait()
    for index, (array, gain, normed, full) in enumerate(((k_in, k_gain, kn, k_all), (q_in, q_gain, qn, q_all))):
        total = jnp.sum(squares[index] + squares_in[index], axis=1, keepdims=True)
        inverse = lax.rsqrt(total / (features * subs) + EPSILON)
        for head in range(features // HD):
            here = slice(head * HD, (head + 1) * HD)
            normed[head] = (array[:, here].astype(F32) * inverse * gain[:, here]).astype(BF16)
        to_peers(1 + index, 1, n)
        full[own, :] = normed[z]
    v_all[own, :] = v_in[:, pl.ds(pl.multiple_of(z * HD, HD), HD)]
    positions = lax.broadcasted_iota(jnp.int32, bias.shape, 1)
    bias[...] = jnp.where(positions < count[0], 0.0, -1e30)

    weight_load.wait()

    def ring(k, upwards, chunk):
        plane = (z - k + n) % n if upwards else (z + k) % n
        start = plane * share + sum(CUTS[:chunk])
        rows = w_ring.at[pl.ds(pl.multiple_of(start, 16), CUTS[chunk]), :]
        to = (z + 1) % n if upwards else (z + n - 1) % n
        lane = 2 * chunk + upwards
        send, arrive = ring_send.at[lane, k], ring_recv.at[lane, k]
        return remote(rows, rows, send, arrive, {"seq": to})

    ways = [(upwards, chunk, n // 2 - (upwards != (chunk == 0))) for chunk in (0, 1) for upwards in (True, False)]

    def pair_weights(plane):
        row = pl.multiple_of((plane % per_half) * share, 16)
        return remote(w_ring.at[pl.ds(pl.multiple_of(plane * share, 16), share), :], w_pair.at[pl.ds(row, share), :],
                      w_send.at[plane % per_half], w_recv.at[plane % per_half], {"sub": 1 - s})

    def have(plane):
        @pl.when(plane // per_half != s)
        def _():
            pair_weights(plane).start()

    def relay(k):
        if k:
            with jax.named_scope(f"relay{k}"):
                for upwards, chunk, hops in ways:
                    if k <= hops:
                        ring_arrival(k, upwards, chunk).wait_recv()
                    if k < hops:
                        ring(k, upwards, chunk).start()
            have((z + k) % n)
            if 2 * k < n:
                have((z - k + n) % n)
        else:
            for upwards, chunk, hops in ways:
                ring(0, upwards, chunk).start()
            have(z)

    def ring_arrival(k, upwards, chunk):
        plane = (z - k + n) % n if upwards else (z + k) % n
        start = plane * share + sum(CUTS[:chunk])
        rows = w_ring.at[pl.ds(pl.multiple_of(start, 16), CUTS[chunk]), :]
        lane = 2 * chunk + upwards
        return remote(rows, rows, ring_send.at[lane, k - 1], ring_recv.at[lane, k - 1], {"seq": z})

    relay(0)

    def arrived(i, carry):
        d = hop(i)
        for full, send, arrive in ((v_all, v_send, v_recv), (k_all, k_send, k_recv)):
            there = full.at[own, :]
            remote(there, there, send.at[d], arrive.at[d], {"seq": z}).wait_recv()
        return carry

    with jax.named_scope("vk"):
        lax.fori_loop(1, n, arrived, 0)
    factor = math.log2(math.e) / math.sqrt(HD)
    mine = pl.ds(pl.multiple_of((s * MEMBERS + me) * tokens, tokens), tokens)

    def o_copy(d):
        lanes = pl.ds(pl.multiple_of(z * HD, HD), HD)
        return remote(o_out.at[d], att.at[mine, lanes], o_send.at[d], o_recv.at[d], {"seq": (z - d + n) % n})

    def attend(i, carry):
        d = hop(i)
        rows = pl.ds(pl.multiple_of(((z - d + n) % n) * tokens, tokens), tokens)

        @pl.when(i > 0)
        def _():
            there = q_all.at[own, :]
            with jax.named_scope("q"):
                remote(there, there, q_send.at[d], q_recv.at[d], {"seq": z}).wait_recv()

        scores = nt(q_all[rows, :], k_all[...]) * factor + bias[0:1, :]
        weights = jnp.exp2(scores - jnp.max(scores, axis=1, keepdims=True))
        denominator = jnp.sum(weights, axis=1, keepdims=True)
        summed = jnp.dot(weights.astype(BF16), v_all[...], preferred_element_type=F32)
        o_out[d] = (summed / denominator).astype(BF16)

        @pl.when(i > 0)
        def _():
            o_copy(d).start()

        return carry

    def spread(body, first, last, points):
        for stop, k in points:
            lax.fori_loop(first, stop, body, 0)
            relay(k)
            first = stop
        lax.fori_loop(first, last, body, 0)

    with jax.named_scope("attend"):
        spread(attend, 0, n, IN_ATTENTION)
    att[mine, pl.ds(pl.multiple_of(z * HD, HD), HD)] = o_out[0]

    def o_arrived(i, carry):
        o_copy(hop(i)).wait_recv()
        return carry

    with jax.named_scope("o"):
        spread(o_arrived, 1, n, IN_RETURN)

    def block(half, number):
        return att.at[pl.ds(pl.multiple_of((half * MEMBERS + number) * tokens, tokens), tokens), :]

    square_copies, pair_copies = {}, {}
    for e in range(1, MEMBERS):
        square_copies[e] = remote(block(s, me), block(s, me), att_send.at[e], att_recv.at[e], {"groups": square(e)[0]})
        square_copies[e].start()
    for e in range(MEMBERS):
        number = square(e)[1]
        pair_copies[e] = remote(block(s, number), block(s, number), pair_send.at[e], pair_recv.at[e], {"sub": 1 - s})
        if e:
            with jax.named_scope(f"square{e}"):
                square_copies[e].wait_recv()
        pair_copies[e].start()
        if e in IN_SQUARE:
            relay(IN_SQUARE[e])
    for e in range(MEMBERS):
        with jax.named_scope(f"pair{e}"):
            pair_copies[e].wait_recv()

    def gates_arrived(i, carry):
        for e in range(1, MEMBERS):
            gate_copy(i, e).wait_recv()
        return carry

    lax.fori_loop(0, per_half, gates_arrived, 0)

    every = MEMBERS * tokens

    def half_att(half):
        return att[pl.ds(pl.multiple_of(half * every, HD), every), :]

    def out_copy(i, e):
        there, number = square(e)
        return remote(result.at[pl.ds(pl.multiple_of((number * per_half + i) * share, 16), share), :],
                      out.at[gate_rows(i, me), :], out_send.at[i, e], out_recv.at[i, e], {"groups": there})

    def project(j, carry):
        plane = (z + hop(j)) % n
        i = plane % per_half

        @pl.when(plane // per_half == s)
        def _():
            with jax.named_scope("pairw"):
                pair_weights(plane).wait_recv()
            with jax.named_scope("project"):
                total = nt(w_ring[pl.ds(pl.multiple_of(plane * share, 16), share), :], half_att(s))
                total = total + nt(w_pair[pl.ds(pl.multiple_of(i * share, 16), share), :], half_att(1 - s))
                for number in range(MEMBERS):
                    rows = pl.ds(pl.multiple_of((number * per_half + i) * share, 16), share)
                    result[rows, :] = (total[:, number * tokens : (number + 1) * tokens] * gates[rows, :]).astype(BF16)
            for e in range(1, MEMBERS):
                out_copy(i, e).start()
            out[gate_rows(i, me), :] = result[pl.ds(pl.multiple_of((me * per_half + i) * share, 16), share), :]

        return carry

    spread(project, 0, n, IN_PROJECTION)

    def sent(i, carry):
        d = hop(i)
        there = k_all.at[own, :]
        for send, arrive in ((v_send, v_recv), (k_send, k_recv), (q_send, q_recv)):
            remote(there, there, send.at[d], arrive.at[d], {"seq": z}).wait_send()
        o_copy(d).wait_send()
        return carry

    lax.fori_loop(1, n, sent, 0)

    for upwards, chunk, hops in ways:
        for k in range(hops):
            ring(k, upwards, chunk).wait_send()

    def finished(i, carry):
        pair_weights((1 - s) * per_half + i).wait_send()
        for e in range(1, MEMBERS):
            gate_copy(i, e).wait_send()
            out_copy(i, e).wait()
        return carry

    for copy in list(square_copies.values()) + list(pair_copies.values()):
        copy.wait_send()
    with jax.named_scope("out"):
        lax.fori_loop(0, per_half, finished, 0)


def shards(n, groups, subs, q, k, v, weight, q_gain, k_gain, gate, count):
    tokens, features = q.shape
    width = weight.shape[1]
    share, per_half = width // MEMBERS, n // subs
    vmem = pl.BlockSpec(memory_space=pltpu.VMEM)
    hbm = pl.BlockSpec(memory_space=pl.ANY)
    dma = pltpu.SemaphoreType.DMA
    rows = n * tokens
    return pl.pallas_call(
        functools.partial(kernel, n, math.isqrt(groups), subs),
        out_shape=jax.ShapeDtypeStruct((per_half * width, tokens), BF16),
        in_specs=[hbm] * 4 + [vmem] * 3 + [pl.BlockSpec(memory_space=pltpu.SMEM)],
        out_specs=vmem,
        scratch_shapes=[
            pltpu.VMEM((tokens, features), BF16),
            pltpu.VMEM((tokens, features), BF16),
            pltpu.VMEM((tokens, features), BF16),
            pltpu.VMEM((per_half * width, HD), F32),
            pltpu.VMEM((2, tokens, HD), F32),
            pltpu.VMEM((2, tokens, HD), F32),
            pltpu.VMEM((n, tokens, HD), BF16),
            pltpu.VMEM((n, tokens, HD), BF16),
            pltpu.VMEM((rows, HD), BF16),
            pltpu.VMEM((rows, HD), BF16),
            pltpu.VMEM((rows, HD), BF16),
            pltpu.VMEM((8, rows), F32),
            pltpu.VMEM((n, tokens, HD), BF16),
            pltpu.VMEM((subs * MEMBERS * tokens, features), BF16),
            pltpu.VMEM((n * share, features), BF16),
            pltpu.VMEM((per_half * share, features), BF16),
            pltpu.VMEM((MEMBERS * per_half * share, HD), F32),
            pltpu.VMEM((MEMBERS * per_half * share, tokens), BF16),
            dma((4,)),
        ]
        + [dma((n,))] * 8
        + [dma((4, n // 2))] * 2
        + [dma((per_half,))] * 2
        + [dma((1,))] * 2
        + [dma((per_half, MEMBERS))] * 2
        + [dma((MEMBERS,))] * 4
        + [dma((per_half, MEMBERS))] * 2,
        compiler_params=pltpu.CompilerParams(
            collective_id=0, has_side_effects=True, vmem_limit_bytes=56 * 2**20
        ),
        name="attention",
    )(q, k, v, weight.T, q_gain.reshape(1, -1), k_gain.reshape(1, -1), gate, count).T


def solution(mesh):
    placed = (
        P(("groups", "seq"), "sub"),
        P(("groups", "seq"), "sub"),
        P(("groups", "seq"), "sub"),
        P("sub", "seq"),
        P("sub"),
        P("sub"),
        P(("groups", "sub")),
        P("groups"),
    )
    return jax.shard_map(
        functools.partial(shards, mesh.shape["seq"], mesh.shape["groups"], mesh.shape["sub"]),
        mesh=mesh,
        in_specs=placed,
        out_specs=P(("groups", "seq"), "sub"),
        check_vma=False,
    )
```

```python
import functools
import math

import jax
import jax.numpy as jnp
from jax import lax
from jax.experimental import pallas as pl
from jax.experimental.pallas import tpu as pltpu
from jax.sharding import PartitionSpec as P

HD = 128
EPSILON = 1e-06
MEMBERS = 4
CUTS = (48, 32)
IN_ATTENTION = ((6, 0), (16, 1))
IN_SQUARE = {0: 2}
IN_PROJECTION = ((5, 3), (7, 4), (9, 5), (11, 6), (13, 7), (15, 8))
F32, BF16 = jnp.float32, jnp.bfloat16


def remote(source, target, send, arrive, where):
    return pltpu.make_async_remote_copy(
        src_ref=source,
        dst_ref=target,
        send_sem=send,
        recv_sem=arrive,
        device_id=where,
        device_id_type=pl.DeviceIdType.MESH,
    )


def nt(left, right):
    return lax.dot_general(left, right, (((1,), (1,)), ((), ())), preferred_element_type=F32)


def kernel(
    n, side, subs,
    q_any, k_any, v_any, w_any, q_gain_any, k_gain_any, gate_any, count,
    out,
    q_in, k_in, v_in, q_gain, k_gain, gate_in, gate_turned, squares, squares_in, kn, qn, k_all, v_all, q_all, bias, o_out,
    att, w_ring, w_pair, gates, result,
    load, sends, v_recv, k_recv, q_recv, o_recv,
    ring_recv, w_recv, small_recv, gate_recv, att_recv, pair_recv, out_recv, out_own,
):
    tokens, features = q_in.shape
    share = w_any.shape[0] // MEMBERS
    per_half = n // subs
    z = lax.axis_index("seq")
    s = lax.axis_index("sub")
    g = lax.axis_index("groups")
    gx, gy = g % side, g // side
    bx, by = gx % 2, gy % 2
    me = 2 * by + bx

    def square(e):
        there = g + (e % 2) * (1 - 2 * bx) + (e // 2) * side * (1 - 2 * by)
        return there, 2 * ((by + e // 2) % 2) + (bx + e) % 2

    def hop(i):
        return (i % 2) * ((i + 1) // 2) + (1 - i % 2) * ((n - i // 2) % n)

    barrier = pltpu.get_barrier_semaphore()

    def greet(i, carry):
        pl.semaphore_signal(barrier, inc=1, device_id={"seq": (z + hop(n - i)) % n}, device_id_type=pl.DeviceIdType.MESH)
        return carry

    lax.fori_loop(1, n, greet, 0)
    pl.semaphore_signal(barrier, inc=1, device_id={"sub": 1 - s}, device_id_type=pl.DeviceIdType.MESH)
    for e in range(1, MEMBERS):
        pl.semaphore_signal(barrier, inc=1, device_id={"groups": square(e)[0]}, device_id_type=pl.DeviceIdType.MESH)

    loads = [
        pltpu.make_async_copy(source, target, load.at[index])
        for index, (source, target) in enumerate((
            (k_any, k_in), (q_any, q_in), (v_any, v_in), (k_gain_any, k_gain), (q_gain_any, q_gain), (gate_any, gate_in),
        ))
    ]
    for copy in loads:
        copy.start()

    for index, array in enumerate((k_in, q_in)):
        loads[index].wait()
        total = jnp.zeros((tokens, HD), F32)
        for head in range(features // HD):
            wide = array[:, head * HD : (head + 1) * HD].astype(F32)
            total = total + wide * wide
        squares[index] = total

    weight_load = pltpu.make_async_copy(
        w_any.at[pl.ds(pl.multiple_of(me * share, 16), share), :],
        w_ring.at[pl.ds(pl.multiple_of(z * share, 16), share), :],
        load.at[6],
    )
    weight_load.start()

    loads[2].wait()
    with jax.named_scope("barrier"):
        pl.semaphore_wait(barrier, n - 1 + 1 + MEMBERS - 1)

    pair = remote(squares, squares_in, sends.at[1], small_recv.at[0], {"sub": 1 - s})
    pair.start()

    own = pl.ds(pl.multiple_of(z * tokens, tokens), tokens)

    def v_block(there):
        return v_in.at[:, pl.ds(pl.multiple_of(there * HD, HD), HD)]

    exchanges = (
        (v_block, v_all, lambda d: v_recv.at[0]),
        (lambda there: kn.at[there], k_all, lambda d: k_recv.at[0]),
        (lambda there: qn.at[there], q_all, lambda d: q_recv.at[d]),
    )

    def to_peers(array, first, last):
        source, target, arrive = exchanges[array]

        def one(i, carry):
            d = hop(i)
            there = (z + d) % n
            remote(source(there), target.at[own, :], sends.at[0], arrive(d), {"seq": there}).start()
            return carry

        lax.fori_loop(first, last, one, 0)

    to_peers(0, 1, n)

    loads[5].wait()
    gate = gate_in[...].reshape(1, gate_in.shape[0])
    for first in range(0, gate_in.shape[0], HD):
        gate_turned[first : first + HD, :] = jnp.transpose(jnp.broadcast_to(gate[:, first : first + HD], (HD, HD)))
    def gate_rows(i, number):
        return pl.ds(pl.multiple_of((i * MEMBERS + number) * share, 16), share)

    def gate_copy(i, e):
        there, number = square(e)
        return remote(gate_turned.at[gate_rows(i, number), :],
                      gates.at[pl.ds(pl.multiple_of((me * per_half + i) * share, 16), share), :],
                      sends.at[2], gate_recv.at[0], {"groups": there})

    def gate_out(i, carry):
        for e in range(1, MEMBERS):
            gate_copy(i, e).start()
        gates[pl.ds(pl.multiple_of((me * per_half + i) * share, 16), share), :] = gate_turned[gate_rows(i, me), :]
        return carry

    lax.fori_loop(0, per_half, gate_out, 0)

    pair.wait_recv()
    loads[3].wait()
    loads[4].wait()
    for index, (array, gain, normed, full) in enumerate(((k_in, k_gain, kn, k_all), (q_in, q_gain, qn, q_all))):
        total = jnp.sum(squares[index] + squares_in[index], axis=1, keepdims=True)
        inverse = lax.rsqrt(total / (features * subs) + EPSILON)
        for head in range(features // HD):
            here = slice(head * HD, (head + 1) * HD)
            normed[head] = (array[:, here].astype(F32) * inverse * gain[:, here]).astype(BF16)
        to_peers(1 + index, 1, n)
        full[own, :] = normed[z]
    v_all[own, :] = v_in[:, pl.ds(pl.multiple_of(z * HD, HD), HD)]
    positions = lax.broadcasted_iota(jnp.int32, bias.shape, 1)
    bias[...] = jnp.where(positions < count[0], 0.0, -1e30)

    weight_load.wait()

    def ring(k, upwards, chunk):
        plane = (z - k + n) % n if upwards else (z + k) % n
        start = plane * share + sum(CUTS[:chunk])
        rows = w_ring.at[pl.ds(pl.multiple_of(start, 16), CUTS[chunk]), :]
        to = (z + 1) % n if upwards else (z + n - 1) % n
        lane = 2 * chunk + upwards
        return remote(rows, rows, sends.at[3], ring_recv.at[lane, k], {"seq": to})

    ways = [(upwards, chunk, n // 2 - (upwards != (chunk == 0))) for chunk in (0, 1) for upwards in (True, False)]

    def pair_weights(plane):
        row = pl.multiple_of((plane % per_half) * share, 16)
        return remote(w_ring.at[pl.ds(pl.multiple_of(plane * share, 16), share), :], w_pair.at[pl.ds(row, share), :],
                      sends.at[4], w_recv.at[plane % per_half], {"sub": 1 - s})

    def have(plane):
        @pl.when(plane // per_half != s)
        def _():
            pair_weights(plane).start()

    def relay(k):
        if k:
            with jax.named_scope(f"relay{k}"):
                for upwards, chunk, hops in ways:
                    if k <= hops:
                        ring_arrival(k, upwards, chunk).wait_recv()
                    if k < hops:
                        ring(k, upwards, chunk).start()
            have((z + k) % n)
            if 2 * k < n:
                have((z - k + n) % n)
        else:
            for upwards, chunk, hops in ways:
                ring(0, upwards, chunk).start()
            have(z)

    def ring_arrival(k, upwards, chunk):
        plane = (z - k + n) % n if upwards else (z + k) % n
        start = plane * share + sum(CUTS[:chunk])
        rows = w_ring.at[pl.ds(pl.multiple_of(start, 16), CUTS[chunk]), :]
        lane = 2 * chunk + upwards
        return remote(rows, rows, sends.at[3], ring_recv.at[lane, k - 1], {"seq": z})

    def whole(array, arrive):
        there = array.at[pl.ds(0, (n - 1) * tokens), :]
        return remote(there, there, sends.at[0], arrive.at[0], {"seq": z})

    with jax.named_scope("vk"):
        whole(v_all, v_recv).wait_recv()
        whole(k_all, k_recv).wait_recv()
    factor = math.log2(math.e) / math.sqrt(HD)
    mine = pl.ds(pl.multiple_of((s * MEMBERS + me) * tokens, tokens), tokens)

    def o_copy(d):
        lanes = pl.ds(pl.multiple_of(z * HD, HD), HD)
        return remote(o_out.at[d], att.at[mine, lanes], sends.at[0], o_recv.at[d], {"seq": (z - d + n) % n})

    def attend(i, carry):
        d = hop(i)
        rows = pl.ds(pl.multiple_of(((z - d + n) % n) * tokens, tokens), tokens)

        @pl.when(i > 0)
        def _():
            there = q_all.at[own, :]
            with jax.named_scope("q"):
                remote(there, there, sends.at[0], q_recv.at[d], {"seq": z}).wait_recv()

        scores = nt(q_all[rows, :], k_all[...]) * factor + bias[0:1, :]
        weights = jnp.exp2(scores - jnp.max(scores, axis=1, keepdims=True))
        denominator = jnp.sum(weights, axis=1, keepdims=True)
        summed = jnp.dot(weights.astype(BF16), v_all[...], preferred_element_type=F32)
        o_out[d] = (summed / denominator).astype(BF16)

        @pl.when(i > 0)
        def _():
            o_copy(d).start()

        return carry

    def spread(body, first, last, points):
        for stop, k in points:
            lax.fori_loop(first, stop, body, 0)
            relay(k)
            first = stop
        lax.fori_loop(first, last, body, 0)

    with jax.named_scope("attend"):
        spread(attend, 0, n, IN_ATTENTION)
    att[mine, pl.ds(pl.multiple_of(z * HD, HD), HD)] = o_out[0]

    def square_copy(d, e):
        lanes = pl.ds(pl.multiple_of(((z + d) % n) * HD, HD), HD)
        return remote(att.at[mine, lanes], att.at[mine, lanes], sends.at[5], att_recv.at[e], {"groups": square(e)[0]})

    def o_arrived(i, carry):
        d = hop(i)

        @pl.when(i > 0)
        def _():
            o_copy(d).wait_recv()

        for e in range(1, MEMBERS):
            square_copy(d, e).start()
        return carry

    with jax.named_scope("o"):
        lax.fori_loop(0, n, o_arrived, 0)

    def block(half, number):
        return att.at[pl.ds(pl.multiple_of((half * MEMBERS + number) * tokens, tokens), tokens), :]

    pair_copies = {}
    for e in range(MEMBERS):
        number = square(e)[1]
        pair_copies[e] = remote(block(s, number), block(s, number), sends.at[6], pair_recv.at[e], {"sub": 1 - s})
        if e:
            with jax.named_scope(f"square{e}"):
                remote(block(s, number), block(s, number), sends.at[5], att_recv.at[e], {"sub": s}).wait_recv()
        pair_copies[e].start()
        if e in IN_SQUARE:
            relay(IN_SQUARE[e])
    for e in range(MEMBERS):
        with jax.named_scope(f"pair{e}"):
            pair_copies[e].wait_recv()

    others = (MEMBERS - 1) * per_half * share

    def all_gates():
        there = gates.at[pl.ds(0, others), :]
        return remote(there, there, sends.at[2], gate_recv.at[0], {"seq": z})

    all_gates().wait_recv()

    every = MEMBERS * tokens

    def half_att(half):
        return att[pl.ds(pl.multiple_of(half * every, HD), every), :]

    def out_copy(i, e):
        there, number = square(e)
        return remote(result.at[pl.ds(pl.multiple_of((number * per_half + i) * share, 16), share), :],
                      out.at[gate_rows(i, me), :], sends.at[7], out_recv.at[0], {"groups": there})

    def own_out(i):
        rows = pl.ds(pl.multiple_of((me * per_half + i) * share, 16), share)
        return pltpu.make_async_copy(result.at[rows, :], out.at[gate_rows(i, me), :], out_own.at[0])

    def project(j, carry):
        plane = (z + hop(j)) % n
        i = plane % per_half

        @pl.when(plane // per_half == s)
        def _():
            with jax.named_scope("pairw"):
                pair_weights(plane).wait_recv()
            with jax.named_scope("project"):
                total = nt(w_ring[pl.ds(pl.multiple_of(plane * share, 16), share), :], half_att(s))
                total = total + nt(w_pair[pl.ds(pl.multiple_of(i * share, 16), share), :], half_att(1 - s))
                for number in range(MEMBERS):
                    rows = pl.ds(pl.multiple_of((number * per_half + i) * share, 16), share)
                    result[rows, :] = (total[:, number * tokens : (number + 1) * tokens] * gates[rows, :]).astype(BF16)
            for e in range(1, MEMBERS):
                out_copy(i, e).start()
            own_out(i).start()

        return carry

    spread(project, 0, n, IN_PROJECTION)

    def all_sent(array, rows, index):
        there = array.at[pl.ds(0, rows), :]
        remote(there, there, sends.at[index], small_recv.at[0], {"seq": z}).wait_send()

    peers = (n - 1) * tokens * HD // features
    all_sent(att, 4 * peers, 0)
    pair.wait_send()
    all_gates().wait_send()
    all_sent(w_ring, (n - 1) * share, 3)
    all_sent(w_pair, per_half * share, 4)
    all_sent(att, (MEMBERS - 1) * tokens, 5)
    all_sent(att, MEMBERS * tokens, 6)
    all_sent(result, others, 7)
    with jax.named_scope("out"):
        there = out.at[pl.ds(0, others), :]
        remote(there, there, sends.at[7], out_recv.at[0], {"seq": z}).wait_recv()
        mine_out = out.at[pl.ds(0, per_half * share), :]
        pltpu.make_async_copy(result.at[pl.ds(0, per_half * share), :], mine_out, out_own.at[0]).wait()


def shards(n, groups, subs, q, k, v, weight, q_gain, k_gain, gate, count):
    tokens, features = q.shape
    width = weight.shape[1]
    share, per_half = width // MEMBERS, n // subs
    hbm = pl.BlockSpec(memory_space=pl.ANY)
    dma = pltpu.SemaphoreType.DMA
    rows = n * tokens
    return pl.pallas_call(
        functools.partial(kernel, n, math.isqrt(groups), subs),
        out_shape=jax.ShapeDtypeStruct((per_half * width, tokens), BF16),
        in_specs=[hbm] * 7 + [pl.BlockSpec(memory_space=pltpu.SMEM)],
        out_specs=hbm,
        scratch_shapes=[
            pltpu.VMEM((tokens, features), BF16),
            pltpu.VMEM((tokens, features), BF16),
            pltpu.VMEM((tokens, features), BF16),
            pltpu.VMEM((1, features), F32),
            pltpu.VMEM((1, features), F32),
            pltpu.VMEM((per_half * width,), F32),
            pltpu.VMEM((per_half * width, HD), F32),
            pltpu.VMEM((2, tokens, HD), F32),
            pltpu.VMEM((2, tokens, HD), F32),
            pltpu.VMEM((n, tokens, HD), BF16),
            pltpu.VMEM((n, tokens, HD), BF16),
            pltpu.VMEM((rows, HD), BF16),
            pltpu.VMEM((rows, HD), BF16),
            pltpu.VMEM((rows, HD), BF16),
            pltpu.VMEM((8, rows), F32),
            pltpu.VMEM((n, tokens, HD), BF16),
            pltpu.VMEM((subs * MEMBERS * tokens, features), BF16),
            pltpu.VMEM((n * share, features), BF16),
            pltpu.VMEM((per_half * share, features), BF16),
            pltpu.VMEM((MEMBERS * per_half * share, HD), F32),
            pltpu.VMEM((MEMBERS * per_half * share, tokens), BF16),
            dma((7,)),
            dma((8,)),
            dma((1,)),
            dma((1,)),
            dma((n,)),
            dma((n,)),
            dma((4, n // 2)),
            dma((per_half,)),
            dma((1,)),
            dma((1,)),
            dma((MEMBERS,)),
            dma((MEMBERS,)),
            dma((1,)),
            dma((1,)),
        ],
        compiler_params=pltpu.CompilerParams(
            collective_id=0, has_side_effects=True, vmem_limit_bytes=56 * 2**20
        ),
        name="attention",
    )(q, k, v, weight.T, q_gain.reshape(1, -1), k_gain.reshape(1, -1), gate, count).T


def solution(mesh):
    placed = (
        P(("groups", "seq"), "sub"),
        P(("groups", "seq"), "sub"),
        P(("groups", "seq"), "sub"),
        P("sub", "seq"),
        P("sub"),
        P("sub"),
        P(("groups", "sub")),
        P("groups"),
    )
    return jax.shard_map(
        functools.partial(shards, mesh.shape["seq"], mesh.shape["groups"], mesh.shape["sub"]),
        mesh=mesh,
        in_specs=placed,
        out_specs=P(("groups", "seq"), "sub"),
        check_vma=False,
    )
```

```python
import functools
import math

import jax
import jax.numpy as jnp
from jax import lax
from jax.experimental import pallas as pl
from jax.experimental.pallas import tpu as pltpu
from jax.sharding import PartitionSpec as P

HD = 128
EPSILON = 1e-06
MEMBERS = 4
CUTS = (48, 32)
IN_ATTENTION = ((6, 0), (16, 1))
IN_SQUARE = {1: 2}
IN_PROJECTION = ((5, 3), (7, 4), (9, 5), (11, 6), (13, 7))
F32, BF16 = jnp.float32, jnp.bfloat16


def remote(source, target, send, arrive, where):
    return pltpu.make_async_remote_copy(
        src_ref=source,
        dst_ref=target,
        send_sem=send,
        recv_sem=arrive,
        device_id=where,
        device_id_type=pl.DeviceIdType.MESH,
    )


def nt(left, right):
    return lax.dot_general(left, right, (((1,), (1,)), ((), ())), preferred_element_type=F32)


def kernel(
    n, side, subs,
    q_any, k_any, v_any, w_any, q_gain_any, k_gain_any, gate_any, count,
    out,
    q_in, k_in, v_in, q_gain, k_gain, gate_in, gate_turned, squares, squares_in, kn, qn, k_all, v_all, q_all, bias, o_out,
    att, w_ring, partial, other_partial, gates, result,
    load, sends, v_recv, k_recv, q_recv, o_recv,
    ring_recv, small_recv, gate_recv, att_recv, pair_recv, out_recv, out_own,
):
    tokens, features = q_in.shape
    share = w_any.shape[0] // MEMBERS
    per_half = n // subs
    z = lax.axis_index("seq")
    s = lax.axis_index("sub")
    g = lax.axis_index("groups")
    gx, gy = g % side, g // side
    bx, by = gx % 2, gy % 2
    me = 2 * by + bx

    def square(e):
        there = g + (e % 2) * (1 - 2 * bx) + (e // 2) * side * (1 - 2 * by)
        return there, 2 * ((by + e // 2) % 2) + (bx + e) % 2

    def hop(i):
        return (i % 2) * ((i + 1) // 2) + (1 - i % 2) * ((n - i // 2) % n)

    def far(i):
        return hop((n - i) % n)

    barrier = pltpu.get_barrier_semaphore()

    def greet(i, carry):
        pl.semaphore_signal(barrier, inc=1, device_id={"seq": (z + far(i)) % n}, device_id_type=pl.DeviceIdType.MESH)
        return carry

    lax.fori_loop(1, n, greet, 0)
    pl.semaphore_signal(barrier, inc=1, device_id={"sub": 1 - s}, device_id_type=pl.DeviceIdType.MESH)
    for e in range(1, MEMBERS):
        pl.semaphore_signal(barrier, inc=1, device_id={"groups": square(e)[0]}, device_id_type=pl.DeviceIdType.MESH)

    loads = [
        pltpu.make_async_copy(source, target, load.at[index])
        for index, (source, target) in enumerate((
            (v_any, v_in), (k_any, k_in), (q_any, q_in), (k_gain_any, k_gain), (q_gain_any, q_gain), (gate_any, gate_in),
        ))
    ]
    for copy in loads:
        copy.start()

    weight_load = pltpu.make_async_copy(
        w_any.at[pl.ds(pl.multiple_of(me * share, 16), share), :],
        w_ring.at[pl.ds(pl.multiple_of(z * share, 16), share), :],
        load.at[6],
    )
    weight_load.start()

    def ring(k, upwards, chunk):
        plane = (z - k + n) % n if upwards else (z + k) % n
        start = plane * share + sum(CUTS[:chunk])
        rows = w_ring.at[pl.ds(pl.multiple_of(start, 16), CUTS[chunk]), :]
        to = (z + 1) % n if upwards else (z + n - 1) % n
        lane = 2 * chunk + upwards
        return remote(rows, rows, sends.at[3], ring_recv.at[lane, k], {"seq": to})

    ways = [(upwards, chunk, n // 2 - (upwards != (chunk == 0))) for chunk in (0, 1) for upwards in (True, False)]

    def relay(k):
        if k:
            with jax.named_scope(f"relay{k}"):
                for upwards, chunk, hops in ways:
                    if k <= hops:
                        ring_arrival(k, upwards, chunk).wait_recv()
                    if k < hops:
                        ring(k, upwards, chunk).start()
        else:
            for upwards, chunk, hops in ways:
                ring(0, upwards, chunk).start()

    def ring_arrival(k, upwards, chunk):
        plane = (z - k + n) % n if upwards else (z + k) % n
        start = plane * share + sum(CUTS[:chunk])
        rows = w_ring.at[pl.ds(pl.multiple_of(start, 16), CUTS[chunk]), :]
        lane = 2 * chunk + upwards
        return remote(rows, rows, sends.at[3], ring_recv.at[lane, k - 1], {"seq": z})

    loads[0].wait()
    with jax.named_scope("barrier"):
        pl.semaphore_wait(barrier, n - 1 + 1 + MEMBERS - 1)

    own = pl.ds(pl.multiple_of(z * tokens, tokens), tokens)

    def v_block(there):
        return v_in.at[:, pl.ds(pl.multiple_of(there * HD, HD), HD)]

    exchanges = (
        (v_block, v_all, lambda d: v_recv.at[0]),
        (lambda there: kn.at[there], k_all, lambda d: k_recv.at[0]),
        (lambda there: qn.at[there], q_all, lambda d: q_recv.at[d]),
    )

    def to_peers(array, first, last):
        source, target, arrive = exchanges[array]

        def one(i, carry):
            d = hop(i)
            there = (z + d) % n
            remote(source(there), target.at[own, :], sends.at[0], arrive(d), {"seq": there}).start()
            return carry

        lax.fori_loop(first, last, one, 0)

    weight_load.wait()
    to_peers(0, 1, n)

    for index, array in enumerate((k_in, q_in)):
        loads[1 + index].wait()
        total = jnp.zeros((tokens, HD), F32)
        for head in range(features // HD):
            wide = array[:, head * HD : (head + 1) * HD].astype(F32)
            total = total + wide * wide
        squares[index] = total

    pair = remote(squares, squares_in, sends.at[1], small_recv.at[0], {"sub": 1 - s})
    pair.start()

    loads[5].wait()
    gate = gate_in[...].reshape(1, gate_in.shape[0])
    for first in range(0, gate_in.shape[0], HD):
        gate_turned[first : first + HD, :] = jnp.transpose(jnp.broadcast_to(gate[:, first : first + HD], (HD, HD)))
    def gate_rows(i, number):
        return pl.ds(pl.multiple_of((i * MEMBERS + number) * share, 16), share)

    def gate_copy(i, e):
        there, number = square(e)
        return remote(gate_turned.at[gate_rows(i, number), :],
                      gates.at[pl.ds(pl.multiple_of((me * per_half + i) * share, 16), share), :],
                      sends.at[2], gate_recv.at[0], {"groups": there})

    def gate_out(i, carry):
        for e in range(1, MEMBERS):
            gate_copy(i, e).start()
        gates[pl.ds(pl.multiple_of((me * per_half + i) * share, 16), share), :] = gate_turned[gate_rows(i, me), :]
        return carry

    lax.fori_loop(0, per_half, gate_out, 0)

    pair.wait_recv()
    loads[3].wait()
    loads[4].wait()
    for index, (array, gain, normed, full) in enumerate(((k_in, k_gain, kn, k_all), (q_in, q_gain, qn, q_all))):
        total = jnp.sum(squares[index] + squares_in[index], axis=1, keepdims=True)
        inverse = lax.rsqrt(total / (features * subs) + EPSILON)
        for head in range(features // HD):
            here = slice(head * HD, (head + 1) * HD)
            normed[head] = (array[:, here].astype(F32) * inverse * gain[:, here]).astype(BF16)
        to_peers(1 + index, 1, n)
        full[own, :] = normed[z]
    v_all[own, :] = v_in[:, pl.ds(pl.multiple_of(z * HD, HD), HD)]
    positions = lax.broadcasted_iota(jnp.int32, bias.shape, 1)
    bias[...] = jnp.where(positions < count[0], 0.0, -1e30)

    def whole(array, arrive):
        there = array.at[pl.ds(0, (n - 1) * tokens), :]
        return remote(there, there, sends.at[0], arrive.at[0], {"seq": z})

    with jax.named_scope("vk"):
        whole(v_all, v_recv).wait_recv()
        whole(k_all, k_recv).wait_recv()
    factor = math.log2(math.e) / math.sqrt(HD)
    mine = pl.ds(pl.multiple_of(me * tokens, tokens), tokens)

    def o_copy(d):
        lanes = pl.ds(pl.multiple_of(z * HD, HD), HD)
        return remote(o_out.at[d], att.at[mine, lanes], sends.at[0], o_recv.at[d], {"seq": (z - d + n) % n})

    def attend(i, carry):
        d = hop(i)
        rows = pl.ds(pl.multiple_of(((z - d + n) % n) * tokens, tokens), tokens)

        @pl.when(i > 0)
        def _():
            there = q_all.at[own, :]
            with jax.named_scope("q"):
                remote(there, there, sends.at[0], q_recv.at[d], {"seq": z}).wait_recv()

        scores = nt(q_all[rows, :], k_all[...]) * factor + bias[0:1, :]
        weights = jnp.exp2(scores - jnp.max(scores, axis=1, keepdims=True))
        denominator = jnp.sum(weights, axis=1, keepdims=True)
        summed = jnp.dot(weights.astype(BF16), v_all[...], preferred_element_type=F32)
        o_out[d] = (summed / denominator).astype(BF16)

        @pl.when(i > 0)
        def _():
            o_copy(d).start()

        return carry

    def spread(body, first, last, points):
        for stop, k in points:
            lax.fori_loop(first, stop, body, 0)
            relay(k)
            first = stop
        lax.fori_loop(first, last, body, 0)

    with jax.named_scope("attend"):
        spread(attend, 0, n, IN_ATTENTION)
    att[mine, pl.ds(pl.multiple_of(z * HD, HD), HD)] = o_out[0]

    def square_copy(d, e):
        lanes = pl.ds(pl.multiple_of(((z + d) % n) * HD, HD), HD)
        return remote(att.at[mine, lanes], att.at[mine, lanes], sends.at[5], att_recv.at[e], {"groups": square(e)[0]})

    def o_arrived(i, carry):
        d = hop(i)

        @pl.when(i > 0)
        def _():
            o_copy(d).wait_recv()

        for e in range(1, MEMBERS):
            square_copy(d, e).start()
        return carry

    with jax.named_scope("o"):
        lax.fori_loop(0, n, o_arrived, 0)

    for e in range(1, MEMBERS):
        rows = att.at[pl.ds(pl.multiple_of(square(e)[1] * tokens, tokens), tokens), :]
        with jax.named_scope(f"square{e}"):
            remote(rows, rows, sends.at[5], att_recv.at[e], {"sub": s}).wait_recv()
        if e in IN_SQUARE:
            relay(IN_SQUARE[e])
    others = (MEMBERS - 1) * per_half * share

    def all_gates():
        there = gates.at[pl.ds(0, others), :]
        return remote(there, there, sends.at[2], gate_recv.at[0], {"seq": z})

    all_gates().wait_recv()

    def place(i):
        return pl.ds(pl.multiple_of(i * share, 16), share)

    def give(i):
        return remote(partial.at[1, place(i), :], other_partial.at[place(i), :],
                      sends.at[4], pair_recv.at[i], {"sub": 1 - s})

    def out_copy(i, e):
        there, number = square(e)
        return remote(result.at[pl.ds(pl.multiple_of((number * per_half + i) * share, 16), share), :],
                      out.at[gate_rows(i, me), :], sends.at[6], out_recv.at[0], {"groups": there})

    def own_out(i):
        rows = pl.ds(pl.multiple_of((me * per_half + i) * share, 16), share)
        return pltpu.make_async_copy(result.at[rows, :], out.at[gate_rows(i, me), :], out_own.at[0])

    def project(j, carry):
        plane = (z + hop(j)) % n
        i = plane % per_half
        mine = plane // per_half == s
        with jax.named_scope("project"):
            total = nt(w_ring[pl.ds(pl.multiple_of(plane * share, 16), share), :], att[...])
            partial[jnp.where(mine, 0, 1), place(i), :] = total

        @pl.when(jnp.logical_not(mine))
        def _():
            give(i).start()

        @pl.when((j >= 2) & (j < n - 1))
        def _():
            finish(j - 2)

        return carry

    def finish(j):
        plane = (z + hop(j)) % n
        i = plane % per_half

        @pl.when(plane // per_half == s)
        def _():
            with jax.named_scope("pair"):
                give(i).wait_recv()
            for number in range(MEMBERS):
                rows = pl.ds(pl.multiple_of((number * per_half + i) * share, 16), share)
                lanes = slice(number * tokens, (number + 1) * tokens)
                total = partial[0, place(i), lanes] + other_partial[place(i), lanes]
                result[rows, :] = (total * gates[rows, :]).astype(BF16)
            for e in range(1, MEMBERS):
                out_copy(i, e).start()
            own_out(i).start()

    spread(project, 0, n - 1, IN_PROJECTION)
    finish(n - 3)
    finish(n - 2)
    relay(n // 2)
    project(n - 1, 0)
    finish(n - 1)

    def all_sent(array, rows, index):
        there = array.at[pl.ds(0, rows), :]
        remote(there, there, sends.at[index], small_recv.at[0], {"seq": z}).wait_send()

    peers = (n - 1) * tokens * HD // features
    all_sent(w_ring, 4 * peers, 0)
    pair.wait_send()
    all_gates().wait_send()
    all_sent(w_ring, (n - 1) * share, 3)
    all_sent(other_partial, per_half * share, 4)
    all_sent(att, (MEMBERS - 1) * tokens, 5)
    all_sent(result, others, 6)
    with jax.named_scope("out"):
        there = out.at[pl.ds(0, others), :]
        remote(there, there, sends.at[6], out_recv.at[0], {"seq": z}).wait_recv()
        mine_out = out.at[pl.ds(0, per_half * share), :]
        pltpu.make_async_copy(result.at[pl.ds(0, per_half * share), :], mine_out, out_own.at[0]).wait()


def shards(n, groups, subs, q, k, v, weight, q_gain, k_gain, gate, count):
    tokens, features = q.shape
    width = weight.shape[1]
    share, per_half = width // MEMBERS, n // subs
    hbm = pl.BlockSpec(memory_space=pl.ANY)
    dma = pltpu.SemaphoreType.DMA
    rows = n * tokens
    return pl.pallas_call(
        functools.partial(kernel, n, math.isqrt(groups), subs),
        out_shape=jax.ShapeDtypeStruct((per_half * width, tokens), BF16),
        in_specs=[hbm] * 7 + [pl.BlockSpec(memory_space=pltpu.SMEM)],
        out_specs=hbm,
        scratch_shapes=[
            pltpu.VMEM((tokens, features), BF16),
            pltpu.VMEM((tokens, features), BF16),
            pltpu.VMEM((tokens, features), BF16),
            pltpu.VMEM((1, features), F32),
            pltpu.VMEM((1, features), F32),
            pltpu.VMEM((per_half * width,), F32),
            pltpu.VMEM((per_half * width, HD), F32),
            pltpu.VMEM((2, tokens, HD), F32),
            pltpu.VMEM((2, tokens, HD), F32),
            pltpu.VMEM((n, tokens, HD), BF16),
            pltpu.VMEM((n, tokens, HD), BF16),
            pltpu.VMEM((rows, HD), BF16),
            pltpu.VMEM((rows, HD), BF16),
            pltpu.VMEM((rows, HD), BF16),
            pltpu.VMEM((8, rows), F32),
            pltpu.VMEM((n, tokens, HD), BF16),
            pltpu.VMEM((MEMBERS * tokens, features), BF16),
            pltpu.VMEM((n * share, features), BF16),
            pltpu.VMEM((2, per_half * share, MEMBERS * tokens), F32),
            pltpu.VMEM((per_half * share, MEMBERS * tokens), F32),
            pltpu.VMEM((MEMBERS * per_half * share, HD), F32),
            pltpu.VMEM((MEMBERS * per_half * share, tokens), BF16),
            dma((7,)),
            dma((7,)),
            dma((1,)),
            dma((1,)),
            dma((n,)),
            dma((n,)),
            dma((4, n // 2)),
            dma((1,)),
            dma((1,)),
            dma((MEMBERS,)),
            dma((per_half,)),
            dma((1,)),
            dma((1,)),
        ],
        compiler_params=pltpu.CompilerParams(
            collective_id=0, has_side_effects=True, vmem_limit_bytes=56 * 2**20
        ),
        name="attention",
    )(q, k, v, weight.T, q_gain.reshape(1, -1), k_gain.reshape(1, -1), gate, count).T


def solution(mesh):
    placed = (
        P(("groups", "seq"), "sub"),
        P(("groups", "seq"), "sub"),
        P(("groups", "seq"), "sub"),
        P("sub", "seq"),
        P("sub"),
        P("sub"),
        P(("groups", "sub")),
        P("groups"),
    )
    return jax.shard_map(
        functools.partial(shards, mesh.shape["seq"], mesh.shape["groups"], mesh.shape["sub"]),
        mesh=mesh,
        in_specs=placed,
        out_specs=P(("groups", "seq"), "sub"),
        check_vma=False,
    )
```

```python
import functools
import math

import jax
import jax.numpy as jnp
from jax import lax
from jax.experimental import pallas as pl
from jax.experimental.pallas import tpu as pltpu
from jax.sharding import PartitionSpec as P

HD = 128
EPSILON = 1e-06
MEMBERS = 4
CUTS = (48, 32)
IN_ATTENTION = ((6, 0), (16, 1))
IN_SQUARE = {1: 2}
IN_PROJECTION = ((5, 3), (7, 4), (9, 5), (11, 6), (13, 7))
F32, BF16 = jnp.float32, jnp.bfloat16


def remote(source, target, send, arrive, where):
    return pltpu.make_async_remote_copy(
        src_ref=source,
        dst_ref=target,
        send_sem=send,
        recv_sem=arrive,
        device_id=where,
        device_id_type=pl.DeviceIdType.MESH,
    )


def nt(left, right):
    return lax.dot_general(left, right, (((1,), (1,)), ((), ())), preferred_element_type=F32)


def kernel(
    n, side, subs,
    q_any, k_any, v_any, w_any, q_gain_any, k_gain_any, gate_any, count,
    out,
    q_in, k_in, v_in, q_gain, k_gain, gate_in, gate_turned, squares, squares_in, kn, qn, k_all, v_all, q_all, bias, o_out,
    att, w_ring, partial, other_partial, gates, result,
    from_up, from_down, load, sends, v_recv, k_recv, q_recv, o_recv,
    ring_recv, small_recv, gate_recv, att_recv, pair_recv, out_recv, out_own,
):
    tokens, features = q_in.shape
    share = w_any.shape[0] // MEMBERS
    per_half = n // subs
    z = lax.axis_index("seq")
    s = lax.axis_index("sub")
    g = lax.axis_index("groups")
    gx, gy = g % side, g // side
    bx, by = gx % 2, gy % 2
    me = 2 * by + bx

    def square(e):
        there = g + (e % 2) * (1 - 2 * bx) + (e // 2) * side * (1 - 2 * by)
        return there, 2 * ((by + e // 2) % 2) + (bx + e) % 2

    def hop(i):
        return (i % 2) * ((i + 1) // 2) + (1 - i % 2) * ((n - i // 2) % n)

    def far(i):
        return hop((n - i) % n)

    barrier = pltpu.get_barrier_semaphore()

    near = n // 4

    def greet(i, carry):
        pl.semaphore_signal(barrier, inc=1, device_id={"seq": (z + far(i)) % n}, device_id_type=pl.DeviceIdType.MESH)
        return carry

    lax.fori_loop(n - 2 * near, n, greet, 0)
    pl.semaphore_signal(barrier, inc=1, device_id={"sub": 1 - s}, device_id_type=pl.DeviceIdType.MESH)
    for e in range(1, MEMBERS):
        pl.semaphore_signal(barrier, inc=1, device_id={"groups": square(e)[0]}, device_id_type=pl.DeviceIdType.MESH)

    loads = [
        pltpu.make_async_copy(source, target, load.at[index])
        for index, (source, target) in enumerate((
            (v_any, v_in), (k_any, k_in), (q_any, q_in), (k_gain_any, k_gain), (q_gain_any, q_gain), (gate_any, gate_in),
        ))
    ]
    for copy in loads:
        copy.start()

    weight_load = pltpu.make_async_copy(
        w_any.at[pl.ds(pl.multiple_of(me * share, 16), share), :],
        w_ring.at[pl.ds(pl.multiple_of(z * share, 16), share), :],
        load.at[6],
    )
    weight_load.start()

    def ring(k, upwards, chunk):
        plane = (z - k + n) % n if upwards else (z + k) % n
        start = plane * share + sum(CUTS[:chunk])
        rows = w_ring.at[pl.ds(pl.multiple_of(start, 16), CUTS[chunk]), :]
        to = (z + 1) % n if upwards else (z + n - 1) % n
        lane = 2 * chunk + upwards
        return remote(rows, rows, sends.at[3], ring_recv.at[lane, k], {"seq": to})

    ways = [(upwards, chunk, n // 2 - (upwards != (chunk == 0))) for chunk in (0, 1) for upwards in (True, False)]

    def relay(k):
        if k:
            with jax.named_scope(f"relay{k}"):
                for upwards, chunk, hops in ways:
                    if k <= hops:
                        ring_arrival(k, upwards, chunk).wait_recv()
                    if k < hops:
                        ring(k, upwards, chunk).start()
        else:
            for upwards, chunk, hops in ways:
                ring(0, upwards, chunk).start()

    def ring_arrival(k, upwards, chunk):
        plane = (z - k + n) % n if upwards else (z + k) % n
        start = plane * share + sum(CUTS[:chunk])
        rows = w_ring.at[pl.ds(pl.multiple_of(start, 16), CUTS[chunk]), :]
        lane = 2 * chunk + upwards
        return remote(rows, rows, sends.at[3], ring_recv.at[lane, k - 1], {"seq": z})

    loads[0].wait()
    with jax.named_scope("barrier"):
        pl.semaphore_wait(barrier, 2 * near + 1 + MEMBERS - 1)

    own = pl.ds(pl.multiple_of(z * tokens, tokens), tokens)

    def v_block(there):
        return v_in.at[:, pl.ds(pl.multiple_of(there * HD, HD), HD)]

    exchanges = (
        (v_block, v_all, lambda d: v_recv.at[0]),
        (lambda there: kn.at[there], k_all, lambda d: k_recv.at[0]),
        (lambda there: qn.at[there], q_all, lambda d: q_recv.at[d]),
    )

    def to_peers(array, first, last):
        source, target, arrive = exchanges[array]

        def one(i, carry):
            d = hop(i)
            there = (z + d) % n
            remote(source(there), target.at[own, :], sends.at[0], arrive(d), {"seq": there}).start()
            return carry

        lax.fori_loop(first, last, one, 0)

    weight_load.wait()
    pl.semaphore_signal(from_down.at[0], inc=1, device_id={"seq": (z + near) % n}, device_id_type=pl.DeviceIdType.MESH)
    pl.semaphore_signal(from_up.at[0], inc=1, device_id={"seq": (z + n - near) % n}, device_id_type=pl.DeviceIdType.MESH)
    to_peers(0, 1, 1 + 2 * near)
    with jax.named_scope("beyond"):
        pl.semaphore_wait(from_down.at[0], 1)
        pl.semaphore_wait(from_up.at[0], 1)
    to_peers(0, 1 + 2 * near, n)

    for index, array in enumerate((k_in, q_in)):
        loads[1 + index].wait()
        total = jnp.zeros((tokens, HD), F32)
        for head in range(features // HD):
            wide = array[:, head * HD : (head + 1) * HD].astype(F32)
            total = total + wide * wide
        squares[index] = total

    pair = remote(squares, squares_in, sends.at[1], small_recv.at[0], {"sub": 1 - s})
    pair.start()

    loads[5].wait()
    gate = gate_in[...].reshape(1, gate_in.shape[0])
    for first in range(0, gate_in.shape[0], HD):
        gate_turned[first : first + HD, :] = jnp.transpose(jnp.broadcast_to(gate[:, first : first + HD], (HD, HD)))
    def gate_rows(i, number):
        return pl.ds(pl.multiple_of((i * MEMBERS + number) * share, 16), share)

    def gate_copy(i, e):
        there, number = square(e)
        return remote(gate_turned.at[gate_rows(i, number), :],
                      gates.at[pl.ds(pl.multiple_of((me * per_half + i) * share, 16), share), :],
                      sends.at[2], gate_recv.at[0], {"groups": there})

    def gate_out(i, carry):
        for e in range(1, MEMBERS):
            gate_copy(i, e).start()
        gates[pl.ds(pl.multiple_of((me * per_half + i) * share, 16), share), :] = gate_turned[gate_rows(i, me), :]
        return carry

    lax.fori_loop(0, per_half, gate_out, 0)

    pair.wait_recv()
    loads[3].wait()
    loads[4].wait()
    for index, (array, gain, normed, full) in enumerate(((k_in, k_gain, kn, k_all), (q_in, q_gain, qn, q_all))):
        total = jnp.sum(squares[index] + squares_in[index], axis=1, keepdims=True)
        inverse = lax.rsqrt(total / (features * subs) + EPSILON)
        for head in range(features // HD):
            here = slice(head * HD, (head + 1) * HD)
            normed[head] = (array[:, here].astype(F32) * inverse * gain[:, here]).astype(BF16)
        to_peers(1 + index, 1, n)
        full[own, :] = normed[z]
    v_all[own, :] = v_in[:, pl.ds(pl.multiple_of(z * HD, HD), HD)]
    positions = lax.broadcasted_iota(jnp.int32, bias.shape, 1)
    bias[...] = jnp.where(positions < count[0], 0.0, -1e30)

    def whole(array, arrive):
        there = array.at[pl.ds(0, (n - 1) * tokens), :]
        return remote(there, there, sends.at[0], arrive.at[0], {"seq": z})

    with jax.named_scope("vk"):
        whole(v_all, v_recv).wait_recv()
        whole(k_all, k_recv).wait_recv()
    factor = math.log2(math.e) / math.sqrt(HD)
    mine = pl.ds(pl.multiple_of(me * tokens, tokens), tokens)

    def o_copy(d):
        lanes = pl.ds(pl.multiple_of(z * HD, HD), HD)
        return remote(o_out.at[d], att.at[mine, lanes], sends.at[0], o_recv.at[d], {"seq": (z - d + n) % n})

    def attend(i, carry):
        d = hop(i)
        rows = pl.ds(pl.multiple_of(((z - d + n) % n) * tokens, tokens), tokens)

        @pl.when(i > 0)
        def _():
            there = q_all.at[own, :]
            with jax.named_scope("q"):
                remote(there, there, sends.at[0], q_recv.at[d], {"seq": z}).wait_recv()

        scores = nt(q_all[rows, :], k_all[...]) * factor + bias[0:1, :]
        weights = jnp.exp2(scores - jnp.max(scores, axis=1, keepdims=True))
        denominator = jnp.sum(weights, axis=1, keepdims=True)
        summed = jnp.dot(weights.astype(BF16), v_all[...], preferred_element_type=F32)
        o_out[d] = (summed / denominator).astype(BF16)

        @pl.when(i > 0)
        def _():
            o_copy(d).start()

        return carry

    def spread(body, first, last, points):
        for stop, k in points:
            lax.fori_loop(first, stop, body, 0)
            relay(k)
            first = stop
        lax.fori_loop(first, last, body, 0)

    with jax.named_scope("attend"):
        spread(attend, 0, n, IN_ATTENTION)
    att[mine, pl.ds(pl.multiple_of(z * HD, HD), HD)] = o_out[0]

    def square_copy(d, e):
        lanes = pl.ds(pl.multiple_of(((z + d) % n) * HD, HD), HD)
        return remote(att.at[mine, lanes], att.at[mine, lanes], sends.at[5], att_recv.at[e], {"groups": square(e)[0]})

    def o_arrived(i, carry):
        d = hop(i)

        @pl.when(i > 0)
        def _():
            o_copy(d).wait_recv()

        for e in range(1, MEMBERS):
            square_copy(d, e).start()
        return carry

    with jax.named_scope("o"):
        lax.fori_loop(0, n, o_arrived, 0)

    for e in range(1, MEMBERS):
        rows = att.at[pl.ds(pl.multiple_of(square(e)[1] * tokens, tokens), tokens), :]
        with jax.named_scope(f"square{e}"):
            remote(rows, rows, sends.at[5], att_recv.at[e], {"sub": s}).wait_recv()
        if e in IN_SQUARE:
            relay(IN_SQUARE[e])
    others = (MEMBERS - 1) * per_half * share

    def all_gates():
        there = gates.at[pl.ds(0, others), :]
        return remote(there, there, sends.at[2], gate_recv.at[0], {"seq": z})

    all_gates().wait_recv()

    def place(i):
        return pl.ds(pl.multiple_of(i * share, 16), share)

    def give(i):
        return remote(partial.at[1, place(i), :], other_partial.at[place(i), :],
                      sends.at[4], pair_recv.at[i], {"sub": 1 - s})

    def out_copy(i, e):
        there, number = square(e)
        return remote(result.at[pl.ds(pl.multiple_of((number * per_half + i) * share, 16), share), :],
                      out.at[gate_rows(i, me), :], sends.at[6], out_recv.at[0], {"groups": there})

    def own_out(i):
        rows = pl.ds(pl.multiple_of((me * per_half + i) * share, 16), share)
        return pltpu.make_async_copy(result.at[rows, :], out.at[gate_rows(i, me), :], out_own.at[0])

    def project(j, carry):
        plane = (z + hop(j)) % n
        i = plane % per_half
        mine = plane // per_half == s
        with jax.named_scope("project"):
            total = nt(w_ring[pl.ds(pl.multiple_of(plane * share, 16), share), :], att[...])
            partial[jnp.where(mine, 0, 1), place(i), :] = total

        @pl.when(jnp.logical_not(mine))
        def _():
            give(i).start()

        @pl.when((j >= 2) & (j < n - 1))
        def _():
            finish(j - 2)

        return carry

    def finish(j):
        plane = (z + hop(j)) % n
        i = plane % per_half

        @pl.when(plane // per_half == s)
        def _():
            with jax.named_scope("pair"):
                give(i).wait_recv()
            for number in range(MEMBERS):
                rows = pl.ds(pl.multiple_of((number * per_half + i) * share, 16), share)
                lanes = slice(number * tokens, (number + 1) * tokens)
                total = partial[0, place(i), lanes] + other_partial[place(i), lanes]
                result[rows, :] = (total * gates[rows, :]).astype(BF16)
            for e in range(1, MEMBERS):
                out_copy(i, e).start()
            own_out(i).start()

    spread(project, 0, n - 1, IN_PROJECTION)
    relay(n // 2)
    project(n - 1, 0)
    for j in (3, 2, 1):
        finish(n - j)

    def all_sent(array, rows, index):
        there = array.at[pl.ds(0, rows), :]
        remote(there, there, sends.at[index], small_recv.at[0], {"seq": z}).wait_send()

    peers = (n - 1) * tokens * HD // features
    all_sent(w_ring, 4 * peers, 0)
    pair.wait_send()
    all_gates().wait_send()
    all_sent(w_ring, (n - 1) * share, 3)
    all_sent(other_partial, per_half * share, 4)
    all_sent(att, (MEMBERS - 1) * tokens, 5)
    all_sent(result, others, 6)
    with jax.named_scope("out"):
        there = out.at[pl.ds(0, others), :]
        remote(there, there, sends.at[6], out_recv.at[0], {"seq": z}).wait_recv()
        mine_out = out.at[pl.ds(0, per_half * share), :]
        pltpu.make_async_copy(result.at[pl.ds(0, per_half * share), :], mine_out, out_own.at[0]).wait()


def shards(n, groups, subs, q, k, v, weight, q_gain, k_gain, gate, count):
    tokens, features = q.shape
    width = weight.shape[1]
    share, per_half = width // MEMBERS, n // subs
    hbm = pl.BlockSpec(memory_space=pl.ANY)
    dma = pltpu.SemaphoreType.DMA
    rows = n * tokens
    return pl.pallas_call(
        functools.partial(kernel, n, math.isqrt(groups), subs),
        out_shape=jax.ShapeDtypeStruct((per_half * width, tokens), BF16),
        in_specs=[hbm] * 7 + [pl.BlockSpec(memory_space=pltpu.SMEM)],
        out_specs=hbm,
        scratch_shapes=[
            pltpu.VMEM((tokens, features), BF16),
            pltpu.VMEM((tokens, features), BF16),
            pltpu.VMEM((tokens, features), BF16),
            pltpu.VMEM((1, features), F32),
            pltpu.VMEM((1, features), F32),
            pltpu.VMEM((per_half * width,), F32),
            pltpu.VMEM((per_half * width, HD), F32),
            pltpu.VMEM((2, tokens, HD), F32),
            pltpu.VMEM((2, tokens, HD), F32),
            pltpu.VMEM((n, tokens, HD), BF16),
            pltpu.VMEM((n, tokens, HD), BF16),
            pltpu.VMEM((rows, HD), BF16),
            pltpu.VMEM((rows, HD), BF16),
            pltpu.VMEM((rows, HD), BF16),
            pltpu.VMEM((8, rows), F32),
            pltpu.VMEM((n, tokens, HD), BF16),
            pltpu.VMEM((MEMBERS * tokens, features), BF16),
            pltpu.VMEM((n * share, features), BF16),
            pltpu.VMEM((2, per_half * share, MEMBERS * tokens), F32),
            pltpu.VMEM((per_half * share, MEMBERS * tokens), F32),
            pltpu.VMEM((MEMBERS * per_half * share, HD), F32),
            pltpu.VMEM((MEMBERS * per_half * share, tokens), BF16),
            pltpu.SemaphoreType.REGULAR((1,)),
            pltpu.SemaphoreType.REGULAR((1,)),
            dma((7,)),
            dma((7,)),
            dma((1,)),
            dma((1,)),
            dma((n,)),
            dma((n,)),
            dma((4, n // 2)),
            dma((1,)),
            dma((1,)),
            dma((MEMBERS,)),
            dma((per_half,)),
            dma((1,)),
            dma((1,)),
        ],
        compiler_params=pltpu.CompilerParams(
            collective_id=0, has_side_effects=True, vmem_limit_bytes=56 * 2**20
        ),
        name="attention",
    )(q, k, v, weight.T, q_gain.reshape(1, -1), k_gain.reshape(1, -1), gate, count).T


def solution(mesh):
    placed = (
        P(("groups", "seq"), "sub"),
        P(("groups", "seq"), "sub"),
        P(("groups", "seq"), "sub"),
        P("sub", "seq"),
        P("sub"),
        P("sub"),
        P(("groups", "sub")),
        P("groups"),
    )
    return jax.shard_map(
        functools.partial(shards, mesh.shape["seq"], mesh.shape["groups"], mesh.shape["sub"]),
        mesh=mesh,
        in_specs=placed,
        out_specs=P(("groups", "seq"), "sub"),
        check_vma=False,
    )
```

```python
import functools
import math

import jax
import jax.numpy as jnp
from jax import lax
from jax.experimental import pallas as pl
from jax.experimental.pallas import tpu as pltpu
from jax.sharding import PartitionSpec as P

HD = 128
EPSILON = 1e-06
MEMBERS = 4
CUTS = (48, 32)
IN_ATTENTION = ((6, 0), (16, 1))
IN_SQUARE = {1: 2}
IN_PROJECTION = ((5, 3), (7, 4), (9, 5), (11, 6), (13, 7))
F32, BF16 = jnp.float32, jnp.bfloat16


def remote(source, target, send, arrive, where):
    return pltpu.make_async_remote_copy(
        src_ref=source,
        dst_ref=target,
        send_sem=send,
        recv_sem=arrive,
        device_id=where,
        device_id_type=pl.DeviceIdType.MESH,
    )


def nt(left, right):
    return lax.dot_general(left, right, (((1,), (1,)), ((), ())), preferred_element_type=F32)


def kernel(
    n, side, subs,
    q_any, k_any, v_any, w_any, q_gain_any, k_gain_any, gate_any, count,
    out,
    q_in, k_in, v_in, q_gain, k_gain, gate_in, gate_turned, squares, squares_in, kn, qn, k_all, v_all, q_all, bias, o_out,
    att, w_ring, partial, other_partial, gates, result,
    from_up, from_down, load, sends, v_recv, k_recv, q_recv, o_recv,
    ring_recv, small_recv, gate_recv, att_recv, pair_recv, out_recv,
):
    tokens, features = q_in.shape
    share = w_any.shape[0] // MEMBERS
    per_half = n // subs
    z = lax.axis_index("seq")
    s = lax.axis_index("sub")
    g = lax.axis_index("groups")
    gx, gy = g % side, g // side
    bx, by = gx % 2, gy % 2
    me = 2 * by + bx

    def square(e):
        there = g + (e % 2) * (1 - 2 * bx) + (e // 2) * side * (1 - 2 * by)
        return there, 2 * ((by + e // 2) % 2) + (bx + e) % 2

    def hop(i):
        return (i % 2) * ((i + 1) // 2) + (1 - i % 2) * ((n - i // 2) % n)

    def far(i):
        return hop((n - i) % n)

    barrier = pltpu.get_barrier_semaphore()

    near = n // 4

    def greet(i, carry):
        pl.semaphore_signal(barrier, inc=1, device_id={"seq": (z + far(i)) % n}, device_id_type=pl.DeviceIdType.MESH)
        return carry

    lax.fori_loop(n - 2 * near, n, greet, 0)
    pl.semaphore_signal(barrier, inc=1, device_id={"sub": 1 - s}, device_id_type=pl.DeviceIdType.MESH)
    for e in range(1, MEMBERS):
        pl.semaphore_signal(barrier, inc=1, device_id={"groups": square(e)[0]}, device_id_type=pl.DeviceIdType.MESH)

    loads = [
        pltpu.make_async_copy(source, target, load.at[index])
        for index, (source, target) in enumerate((
            (v_any, v_in), (k_any, k_in), (q_any, q_in), (k_gain_any, k_gain), (q_gain_any, q_gain), (gate_any, gate_in),
        ))
    ]
    for copy in loads:
        copy.start()

    weight_load = pltpu.make_async_copy(
        w_any.at[pl.ds(pl.multiple_of(me * share, 16), share), :],
        w_ring.at[pl.ds(pl.multiple_of(z * share, 16), share), :],
        load.at[6],
    )
    weight_load.start()

    def ring(k, upwards, chunk):
        plane = (z - k + n) % n if upwards else (z + k) % n
        start = plane * share + sum(CUTS[:chunk])
        rows = w_ring.at[pl.ds(pl.multiple_of(start, 16), CUTS[chunk]), :]
        to = (z + 1) % n if upwards else (z + n - 1) % n
        lane = 2 * chunk + upwards
        return remote(rows, rows, sends.at[3], ring_recv.at[lane, k], {"seq": to})

    ways = [(upwards, chunk, n // 2 - (upwards != (chunk == 0))) for chunk in (0, 1) for upwards in (True, False)]

    def relay(k):
        if k:
            with jax.named_scope(f"relay{k}"):
                for upwards, chunk, hops in ways:
                    if k <= hops:
                        ring_arrival(k, upwards, chunk).wait_recv()
                    if k < hops:
                        ring(k, upwards, chunk).start()
        else:
            for upwards, chunk, hops in ways:
                ring(0, upwards, chunk).start()

    def ring_arrival(k, upwards, chunk):
        plane = (z - k + n) % n if upwards else (z + k) % n
        start = plane * share + sum(CUTS[:chunk])
        rows = w_ring.at[pl.ds(pl.multiple_of(start, 16), CUTS[chunk]), :]
        lane = 2 * chunk + upwards
        return remote(rows, rows, sends.at[3], ring_recv.at[lane, k - 1], {"seq": z})

    loads[0].wait()
    with jax.named_scope("barrier"):
        pl.semaphore_wait(barrier, 2 * near + 1 + MEMBERS - 1)

    own = pl.ds(pl.multiple_of(z * tokens, tokens), tokens)

    def v_block(there):
        return v_in.at[:, pl.ds(pl.multiple_of(there * HD, HD), HD)]

    exchanges = (
        (v_block, v_all, lambda d: v_recv.at[0]),
        (lambda there: kn.at[there], k_all, lambda d: k_recv.at[0]),
        (lambda there: qn.at[there], q_all, lambda d: q_recv.at[d]),
    )

    def to_peers(array, first, last):
        source, target, arrive = exchanges[array]

        def one(i, carry):
            d = hop(i)
            there = (z + d) % n
            remote(source(there), target.at[own, :], sends.at[0], arrive(d), {"seq": there}).start()
            return carry

        lax.fori_loop(first, last, one, 0)

    weight_load.wait()
    pl.semaphore_signal(from_down.at[0], inc=1, device_id={"seq": (z + near) % n}, device_id_type=pl.DeviceIdType.MESH)
    pl.semaphore_signal(from_up.at[0], inc=1, device_id={"seq": (z + n - near) % n}, device_id_type=pl.DeviceIdType.MESH)
    to_peers(0, 1, 1 + 2 * near)
    with jax.named_scope("beyond"):
        pl.semaphore_wait(from_down.at[0], 1)
        pl.semaphore_wait(from_up.at[0], 1)
    to_peers(0, 1 + 2 * near, n)

    for index, array in enumerate((k_in, q_in)):
        loads[1 + index].wait()
        total = jnp.zeros((tokens, HD), F32)
        for head in range(features // HD):
            wide = array[:, head * HD : (head + 1) * HD].astype(F32)
            total = total + wide * wide
        squares[index] = total

    pair = remote(squares, squares_in, sends.at[1], small_recv.at[0], {"sub": 1 - s})
    pair.start()

    loads[5].wait()
    gate = gate_in[...].reshape(1, gate_in.shape[0])
    for first in range(0, gate_in.shape[0], HD):
        gate_turned[first : first + HD, :] = jnp.transpose(jnp.broadcast_to(gate[:, first : first + HD], (HD, HD)))
    def gate_rows(i, number):
        return pl.ds(pl.multiple_of((i * MEMBERS + number) * share, 16), share)

    def gate_copy(i, e):
        there, number = square(e)
        return remote(gate_turned.at[gate_rows(i, number), :],
                      gates.at[pl.ds(pl.multiple_of((me * per_half + i) * share, 16), share), :],
                      sends.at[2], gate_recv.at[0], {"groups": there})

    def gate_out(i, carry):
        for e in range(1, MEMBERS):
            gate_copy(i, e).start()
        gates[pl.ds(pl.multiple_of((me * per_half + i) * share, 16), share), :] = gate_turned[gate_rows(i, me), :]
        return carry

    lax.fori_loop(0, per_half, gate_out, 0)

    pair.wait_recv()
    loads[3].wait()
    loads[4].wait()
    for index, (array, gain, normed, full) in enumerate(((k_in, k_gain, kn, k_all), (q_in, q_gain, qn, q_all))):
        total = jnp.sum(squares[index] + squares_in[index], axis=1, keepdims=True)
        inverse = lax.rsqrt(total / (features * subs) + EPSILON)
        for head in range(features // HD):
            here = slice(head * HD, (head + 1) * HD)
            normed[head] = (array[:, here].astype(F32) * inverse * gain[:, here]).astype(BF16)
        to_peers(1 + index, 1, n)
        full[own, :] = normed[z]
    v_all[own, :] = v_in[:, pl.ds(pl.multiple_of(z * HD, HD), HD)]
    positions = lax.broadcasted_iota(jnp.int32, bias.shape, 1)
    bias[...] = jnp.where(positions < count[0], 0.0, -1e30)

    def whole(array, arrive):
        there = array.at[pl.ds(0, (n - 1) * tokens), :]
        return remote(there, there, sends.at[0], arrive.at[0], {"seq": z})

    with jax.named_scope("vk"):
        whole(v_all, v_recv).wait_recv()
        whole(k_all, k_recv).wait_recv()
    factor = math.log2(math.e) / math.sqrt(HD)
    mine = pl.ds(pl.multiple_of(me * tokens, tokens), tokens)

    def o_copy(d):
        lanes = pl.ds(pl.multiple_of(z * HD, HD), HD)
        return remote(o_out.at[d], att.at[mine, lanes], sends.at[0], o_recv.at[d], {"seq": (z - d + n) % n})

    def attend(i, carry):
        d = hop(i)
        rows = pl.ds(pl.multiple_of(((z - d + n) % n) * tokens, tokens), tokens)

        @pl.when(i > 0)
        def _():
            there = q_all.at[own, :]
            with jax.named_scope("q"):
                remote(there, there, sends.at[0], q_recv.at[d], {"seq": z}).wait_recv()

        scores = nt(q_all[rows, :], k_all[...]) * factor + bias[0:1, :]
        weights = jnp.exp2(scores - jnp.max(scores, axis=1, keepdims=True))
        denominator = jnp.sum(weights, axis=1, keepdims=True)
        summed = jnp.dot(weights.astype(BF16), v_all[...], preferred_element_type=F32)
        o_out[d] = (summed / denominator).astype(BF16)

        @pl.when(i > 0)
        def _():
            o_copy(d).start()

        return carry

    def spread(body, first, last, points):
        for stop, k in points:
            lax.fori_loop(first, stop, body, 0)
            relay(k)
            first = stop
        lax.fori_loop(first, last, body, 0)

    with jax.named_scope("attend"):
        spread(attend, 0, n, IN_ATTENTION)
    att[mine, pl.ds(pl.multiple_of(z * HD, HD), HD)] = o_out[0]

    def square_copy(d, e):
        lanes = pl.ds(pl.multiple_of(((z + d) % n) * HD, HD), HD)
        return remote(att.at[mine, lanes], att.at[mine, lanes], sends.at[5], att_recv.at[e], {"groups": square(e)[0]})

    def o_arrived(i, carry):
        d = hop(i)

        @pl.when(i > 0)
        def _():
            o_copy(d).wait_recv()

        for e in range(1, MEMBERS):
            square_copy(d, e).start()
        return carry

    with jax.named_scope("o"):
        lax.fori_loop(0, n, o_arrived, 0)

    for e in range(1, MEMBERS):
        rows = att.at[pl.ds(pl.multiple_of(square(e)[1] * tokens, tokens), tokens), :]
        with jax.named_scope(f"square{e}"):
            remote(rows, rows, sends.at[5], att_recv.at[e], {"sub": s}).wait_recv()
        if e in IN_SQUARE:
            relay(IN_SQUARE[e])
    others = (MEMBERS - 1) * per_half * share

    def all_gates():
        there = gates.at[pl.ds(0, others), :]
        return remote(there, there, sends.at[2], gate_recv.at[0], {"seq": z})

    all_gates().wait_recv()

    def place(i):
        return pl.ds(pl.multiple_of(i * share, 16), share)

    def give(i):
        return remote(partial.at[1, place(i), :], other_partial.at[place(i), :],
                      sends.at[4], pair_recv.at[i], {"sub": 1 - s})

    def out_copy(i, e):
        there, number = square(e)
        return remote(result.at[pl.ds(pl.multiple_of((number * per_half + i) * share, 16), share), :],
                      out.at[gate_rows(i, me), :], sends.at[6], out_recv.at[0], {"groups": there})

    def project(j, carry):
        plane = (z + hop(j)) % n
        i = plane % per_half
        mine = plane // per_half == s
        with jax.named_scope("project"):
            total = nt(w_ring[pl.ds(pl.multiple_of(plane * share, 16), share), :], att[...])
            partial[jnp.where(mine, 0, 1), place(i), :] = total

        @pl.when(jnp.logical_not(mine))
        def _():
            give(i).start()

        @pl.when((j >= 2) & (j < n - 1))
        def _():
            finish(j - 2)

        return carry

    def finish(j):
        plane = (z + hop(j)) % n
        i = plane % per_half

        @pl.when(plane // per_half == s)
        def _():
            with jax.named_scope("pair"):
                give(i).wait_recv()
            for number in range(MEMBERS):
                rows = pl.ds(pl.multiple_of((number * per_half + i) * share, 16), share)
                lanes = slice(number * tokens, (number + 1) * tokens)
                total = partial[0, place(i), lanes] + other_partial[place(i), lanes]
                result[rows, :] = (total * gates[rows, :]).astype(BF16)
            for e in range(1, MEMBERS):
                out_copy(i, e).start()
            out[gate_rows(i, me), :] = result[pl.ds(pl.multiple_of((me * per_half + i) * share, 16), share), :]

    spread(project, 0, n - 1, IN_PROJECTION)
    relay(n // 2)
    project(n - 1, 0)
    for j in (3, 2, 1):
        finish(n - j)

    def all_sent(array, rows, index):
        there = array.at[pl.ds(0, rows), :]
        remote(there, there, sends.at[index], small_recv.at[0], {"seq": z}).wait_send()

    peers = (n - 1) * tokens * HD // features
    all_sent(w_ring, 4 * peers, 0)
    pair.wait_send()
    all_gates().wait_send()
    all_sent(w_ring, (n - 1) * share, 3)
    all_sent(other_partial, per_half * share, 4)
    all_sent(att, (MEMBERS - 1) * tokens, 5)
    all_sent(result, others, 6)
    with jax.named_scope("out"):
        there = out.at[pl.ds(0, others), :]
        remote(there, there, sends.at[6], out_recv.at[0], {"seq": z}).wait_recv()


def shards(n, groups, subs, q, k, v, weight, q_gain, k_gain, gate, count):
    tokens, features = q.shape
    width = weight.shape[1]
    share, per_half = width // MEMBERS, n // subs
    hbm = pl.BlockSpec(memory_space=pl.ANY)
    dma = pltpu.SemaphoreType.DMA
    rows = n * tokens
    return pl.pallas_call(
        functools.partial(kernel, n, math.isqrt(groups), subs),
        out_shape=jax.ShapeDtypeStruct((per_half * width, tokens), BF16),
        in_specs=[hbm] * 7 + [pl.BlockSpec(memory_space=pltpu.SMEM)],
        out_specs=pl.BlockSpec(memory_space=pltpu.VMEM),
        scratch_shapes=[
            pltpu.VMEM((tokens, features), BF16),
            pltpu.VMEM((tokens, features), BF16),
            pltpu.VMEM((tokens, features), BF16),
            pltpu.VMEM((1, features), F32),
            pltpu.VMEM((1, features), F32),
            pltpu.VMEM((per_half * width,), F32),
            pltpu.VMEM((per_half * width, HD), F32),
            pltpu.VMEM((2, tokens, HD), F32),
            pltpu.VMEM((2, tokens, HD), F32),
            pltpu.VMEM((n, tokens, HD), BF16),
            pltpu.VMEM((n, tokens, HD), BF16),
            pltpu.VMEM((rows, HD), BF16),
            pltpu.VMEM((rows, HD), BF16),
            pltpu.VMEM((rows, HD), BF16),
            pltpu.VMEM((8, rows), F32),
            pltpu.VMEM((n, tokens, HD), BF16),
            pltpu.VMEM((MEMBERS * tokens, features), BF16),
            pltpu.VMEM((n * share, features), BF16),
            pltpu.VMEM((2, per_half * share, MEMBERS * tokens), F32),
            pltpu.VMEM((per_half * share, MEMBERS * tokens), F32),
            pltpu.VMEM((MEMBERS * per_half * share, HD), F32),
            pltpu.VMEM((MEMBERS * per_half * share, tokens), BF16),
            pltpu.SemaphoreType.REGULAR((1,)),
            pltpu.SemaphoreType.REGULAR((1,)),
            dma((7,)),
            dma((7,)),
            dma((1,)),
            dma((1,)),
            dma((n,)),
            dma((n,)),
            dma((4, n // 2)),
            dma((1,)),
            dma((1,)),
            dma((MEMBERS,)),
            dma((per_half,)),
            dma((1,)),
        ],
        compiler_params=pltpu.CompilerParams(
            collective_id=0, has_side_effects=True, vmem_limit_bytes=40 * 2**20
        ),
        name="attention",
    )(*(pltpu.with_memory_space_constraint(x, pltpu.HBM) for x in (q, k, v, weight.T, q_gain.reshape(1, -1), k_gain.reshape(1, -1), gate)), count).T


def solution(mesh):
    placed = (
        P(("groups", "seq"), "sub"),
        P(("groups", "seq"), "sub"),
        P(("groups", "seq"), "sub"),
        P("sub", "seq"),
        P("sub"),
        P("sub"),
        P(("groups", "sub")),
        P("groups"),
    )
    return jax.shard_map(
        functools.partial(shards, mesh.shape["seq"], mesh.shape["groups"], mesh.shape["sub"]),
        mesh=mesh,
        in_specs=placed,
        out_specs=P(("groups", "seq"), "sub"),
        check_vma=False,
    )
```

```python
import functools
import math

import jax
import jax.numpy as jnp
from jax import lax
from jax.experimental import pallas as pl
from jax.experimental.pallas import tpu as pltpu
from jax.sharding import PartitionSpec as P

HD = 128
EPSILON = 1e-06
MEMBERS = 4
CUTS = (48, 32)
IN_ATTENTION = ((1, 0), (16, 1))
IN_SQUARE = {1: 2}
IN_PROJECTION = ((5, 3), (7, 4), (9, 5), (11, 6), (13, 7))
F32, BF16 = jnp.float32, jnp.bfloat16


def remote(source, target, send, arrive, where):
    return pltpu.make_async_remote_copy(
        src_ref=source,
        dst_ref=target,
        send_sem=send,
        recv_sem=arrive,
        device_id=where,
        device_id_type=pl.DeviceIdType.MESH,
    )


def nt(left, right):
    return lax.dot_general(left, right, (((1,), (1,)), ((), ())), preferred_element_type=F32)


def kernel(
    n, side, subs,
    q_any, k_any, v_any, w_any, q_gain_any, k_gain_any, gate_any, count,
    out,
    q_in, k_in, v_in, q_gain, k_gain, gate_in, gate_turned, squares, squares_in, kn, qn, k_all, v_all, q_all, bias, o_out,
    att, w_ring, partial, other_partial, gates, result,
    from_up, from_down, load, sends, v_recv, k_recv, q_recv, o_recv,
    ring_recv, small_recv, gate_recv, att_recv, pair_recv, out_recv,
):
    tokens, features = q_in.shape
    share = w_any.shape[0] // MEMBERS
    per_half = n // subs
    z = lax.axis_index("seq")
    s = lax.axis_index("sub")
    g = lax.axis_index("groups")
    gx, gy = g % side, g // side
    bx, by = gx % 2, gy % 2
    me = 2 * by + bx

    def square(e):
        there = g + (e % 2) * (1 - 2 * bx) + (e // 2) * side * (1 - 2 * by)
        return there, 2 * ((by + e // 2) % 2) + (bx + e) % 2

    def hop(i):
        return (i % 2) * ((i + 1) // 2) + (1 - i % 2) * ((n - i // 2) % n)

    def far(i):
        return hop((n - i) % n)

    barrier = pltpu.get_barrier_semaphore()

    near = n // 8

    def greet(i, carry):
        pl.semaphore_signal(barrier, inc=1, device_id={"seq": (z + far(i)) % n}, device_id_type=pl.DeviceIdType.MESH)
        return carry

    lax.fori_loop(n - 2 * near, n, greet, 0)
    pl.semaphore_signal(barrier, inc=1, device_id={"sub": 1 - s}, device_id_type=pl.DeviceIdType.MESH)
    for e in range(1, MEMBERS):
        pl.semaphore_signal(barrier, inc=1, device_id={"groups": square(e)[0]}, device_id_type=pl.DeviceIdType.MESH)

    loads = [
        pltpu.make_async_copy(source, target, load.at[index])
        for index, (source, target) in enumerate((
            (v_any, v_in), (k_any, k_in), (q_any, q_in), (k_gain_any, k_gain), (q_gain_any, q_gain), (gate_any, gate_in),
        ))
    ]
    for copy in loads:
        copy.start()

    weight_load = pltpu.make_async_copy(
        w_any.at[pl.ds(pl.multiple_of(me * share, 16), share), :],
        w_ring.at[pl.ds(pl.multiple_of(z * share, 16), share), :],
        load.at[6],
    )
    weight_load.start()

    def ring(k, upwards, chunk):
        plane = (z - k + n) % n if upwards else (z + k) % n
        start = plane * share + sum(CUTS[:chunk])
        rows = w_ring.at[pl.ds(pl.multiple_of(start, 16), CUTS[chunk]), :]
        to = (z + 1) % n if upwards else (z + n - 1) % n
        lane = 2 * chunk + upwards
        return remote(rows, rows, sends.at[3], ring_recv.at[lane, k], {"seq": to})

    ways = [(upwards, chunk, n // 2 - (upwards != (chunk == 0))) for chunk in (0, 1) for upwards in (True, False)]

    def relay(k):
        if k:
            with jax.named_scope(f"relay{k}"):
                for upwards, chunk, hops in ways:
                    if k <= hops:
                        ring_arrival(k, upwards, chunk).wait_recv()
                    if k < hops:
                        ring(k, upwards, chunk).start()
        else:
            for upwards, chunk, hops in ways:
                ring(0, upwards, chunk).start()

    def ring_arrival(k, upwards, chunk):
        plane = (z - k + n) % n if upwards else (z + k) % n
        start = plane * share + sum(CUTS[:chunk])
        rows = w_ring.at[pl.ds(pl.multiple_of(start, 16), CUTS[chunk]), :]
        lane = 2 * chunk + upwards
        return remote(rows, rows, sends.at[3], ring_recv.at[lane, k - 1], {"seq": z})

    loads[0].wait()
    with jax.named_scope("barrier"):
        pl.semaphore_wait(barrier, 2 * near + 1 + MEMBERS - 1)

    own = pl.ds(pl.multiple_of(z * tokens, tokens), tokens)

    def v_block(there):
        return v_in.at[:, pl.ds(pl.multiple_of(there * HD, HD), HD)]

    exchanges = (
        (v_block, v_all, lambda d: v_recv.at[0]),
        (lambda there: kn.at[there], k_all, lambda d: k_recv.at[0]),
        (lambda there: qn.at[there], q_all, lambda d: q_recv.at[d]),
    )

    def to_peers(array, first, last):
        source, target, arrive = exchanges[array]

        def one(i, carry):
            d = hop(i)
            there = (z + d) % n
            remote(source(there), target.at[own, :], sends.at[0], arrive(d), {"seq": there}).start()
            return carry

        lax.fori_loop(first, last, one, 0)

    weight_load.wait()
    for known in range(near, n // 2, near):
        pl.semaphore_signal(from_down.at[0], inc=1, device_id={"seq": (z + near) % n}, device_id_type=pl.DeviceIdType.MESH)
        pl.semaphore_signal(from_up.at[0], inc=1, device_id={"seq": (z + n - near) % n}, device_id_type=pl.DeviceIdType.MESH)
        to_peers(0, 1 + 2 * (known - near), 1 + 2 * known)
        with jax.named_scope("beyond"):
            pl.semaphore_wait(from_down.at[0], 1)
            pl.semaphore_wait(from_up.at[0], 1)
    to_peers(0, 1 + 2 * (n // 2 - near), n)

    for index, array in enumerate((k_in, q_in)):
        loads[1 + index].wait()
        total = jnp.zeros((tokens, HD), F32)
        for head in range(features // HD):
            wide = array[:, head * HD : (head + 1) * HD].astype(F32)
            total = total + wide * wide
        squares[index] = total

    pair = remote(squares, squares_in, sends.at[1], small_recv.at[0], {"sub": 1 - s})
    pair.start()

    loads[5].wait()
    gate = gate_in[...].reshape(1, gate_in.shape[0])
    for first in range(0, gate_in.shape[0], HD):
        gate_turned[first : first + HD, :] = jnp.transpose(jnp.broadcast_to(gate[:, first : first + HD], (HD, HD)))
    def gate_rows(i, number):
        return pl.ds(pl.multiple_of((i * MEMBERS + number) * share, 16), share)

    def gate_copy(i, e):
        there, number = square(e)
        return remote(gate_turned.at[gate_rows(i, number), :],
                      gates.at[pl.ds(pl.multiple_of((me * per_half + i) * share, 16), share), :],
                      sends.at[2], gate_recv.at[0], {"groups": there})

    def gate_out(i, carry):
        for e in range(1, MEMBERS):
            gate_copy(i, e).start()
        gates[pl.ds(pl.multiple_of((me * per_half + i) * share, 16), share), :] = gate_turned[gate_rows(i, me), :]
        return carry

    lax.fori_loop(0, per_half, gate_out, 0)

    pair.wait_recv()
    loads[3].wait()
    loads[4].wait()
    for index, (array, gain, normed, full) in enumerate(((k_in, k_gain, kn, k_all), (q_in, q_gain, qn, q_all))):
        total = jnp.sum(squares[index] + squares_in[index], axis=1, keepdims=True)
        inverse = lax.rsqrt(total / (features * subs) + EPSILON)
        for head in range(features // HD):
            here = slice(head * HD, (head + 1) * HD)
            normed[head] = (array[:, here].astype(F32) * inverse * gain[:, here]).astype(BF16)
        to_peers(1 + index, 1, n)
        full[own, :] = normed[z]
    v_all[own, :] = v_in[:, pl.ds(pl.multiple_of(z * HD, HD), HD)]
    positions = lax.broadcasted_iota(jnp.int32, bias.shape, 1)
    bias[...] = jnp.where(positions < count[0], 0.0, -1e30)

    def whole(array, arrive):
        there = array.at[pl.ds(0, (n - 1) * tokens), :]
        return remote(there, there, sends.at[0], arrive.at[0], {"seq": z})

    with jax.named_scope("vk"):
        whole(v_all, v_recv).wait_recv()
        whole(k_all, k_recv).wait_recv()
    factor = math.log2(math.e) / math.sqrt(HD)
    mine = pl.ds(pl.multiple_of(me * tokens, tokens), tokens)

    def o_copy(d):
        lanes = pl.ds(pl.multiple_of(z * HD, HD), HD)
        return remote(o_out.at[d], att.at[mine, lanes], sends.at[0], o_recv.at[d], {"seq": (z - d + n) % n})

    def attend(i, carry):
        d = hop(i)
        rows = pl.ds(pl.multiple_of(((z - d + n) % n) * tokens, tokens), tokens)

        @pl.when(i > 0)
        def _():
            there = q_all.at[own, :]
            with jax.named_scope("q"):
                remote(there, there, sends.at[0], q_recv.at[d], {"seq": z}).wait_recv()

        scores = nt(q_all[rows, :], k_all[...]) * factor + bias[0:1, :]
        weights = jnp.exp2(scores - jnp.max(scores, axis=1, keepdims=True))
        denominator = jnp.sum(weights, axis=1, keepdims=True)
        summed = jnp.dot(weights.astype(BF16), v_all[...], preferred_element_type=F32)
        o_out[d] = (summed / denominator).astype(BF16)

        @pl.when(i > 0)
        def _():
            o_copy(d).start()

        return carry

    def spread(body, first, last, points):
        for stop, k in points:
            lax.fori_loop(first, stop, body, 0)
            relay(k)
            first = stop
        lax.fori_loop(first, last, body, 0)

    with jax.named_scope("attend"):
        spread(attend, 0, n, IN_ATTENTION)
    att[mine, pl.ds(pl.multiple_of(z * HD, HD), HD)] = o_out[0]

    def square_copy(d, e):
        lanes = pl.ds(pl.multiple_of(((z + d) % n) * HD, HD), HD)
        return remote(att.at[mine, lanes], att.at[mine, lanes], sends.at[5], att_recv.at[e], {"groups": square(e)[0]})

    def o_arrived(i, carry):
        d = hop(i)

        @pl.when(i > 0)
        def _():
            o_copy(d).wait_recv()

        for e in range(1, MEMBERS):
            square_copy(d, e).start()
        return carry

    with jax.named_scope("o"):
        lax.fori_loop(0, n, o_arrived, 0)

    for e in range(1, MEMBERS):
        rows = att.at[pl.ds(pl.multiple_of(square(e)[1] * tokens, tokens), tokens), :]
        with jax.named_scope(f"square{e}"):
            remote(rows, rows, sends.at[5], att_recv.at[e], {"sub": s}).wait_recv()
        if e in IN_SQUARE:
            relay(IN_SQUARE[e])
    others = (MEMBERS - 1) * per_half * share

    def all_gates():
        there = gates.at[pl.ds(0, others), :]
        return remote(there, there, sends.at[2], gate_recv.at[0], {"seq": z})

    all_gates().wait_recv()

    def place(i):
        return pl.ds(pl.multiple_of(i * share, 16), share)

    def give(i):
        return remote(partial.at[1, place(i), :], other_partial.at[place(i), :],
                      sends.at[4], pair_recv.at[i], {"sub": 1 - s})

    def out_copy(i, e):
        there, number = square(e)
        return remote(result.at[pl.ds(pl.multiple_of((number * per_half + i) * share, 16), share), :],
                      out.at[gate_rows(i, me), :], sends.at[6], out_recv.at[0], {"groups": there})

    def project(j, carry):
        plane = (z + hop(j)) % n
        i = plane % per_half
        mine = plane // per_half == s
        with jax.named_scope("project"):
            total = nt(w_ring[pl.ds(pl.multiple_of(plane * share, 16), share), :], att[...])
            partial[jnp.where(mine, 0, 1), place(i), :] = total

        @pl.when(jnp.logical_not(mine))
        def _():
            give(i).start()

        @pl.when((j >= 2) & (j < n - 1))
        def _():
            finish(j - 2)

        return carry

    def finish(j):
        plane = (z + hop(j)) % n
        i = plane % per_half

        @pl.when(plane // per_half == s)
        def _():
            with jax.named_scope("pair"):
                give(i).wait_recv()
            for number in range(MEMBERS):
                rows = pl.ds(pl.multiple_of((number * per_half + i) * share, 16), share)
                lanes = slice(number * tokens, (number + 1) * tokens)
                total = partial[0, place(i), lanes] + other_partial[place(i), lanes]
                result[rows, :] = (total * gates[rows, :]).astype(BF16)
            for e in range(1, MEMBERS):
                out_copy(i, e).start()
            out[gate_rows(i, me), :] = result[pl.ds(pl.multiple_of((me * per_half + i) * share, 16), share), :]

    spread(project, 0, n - 1, IN_PROJECTION)
    relay(n // 2)
    project(n - 1, 0)
    for j in (3, 2, 1):
        finish(n - j)

    def all_sent(array, rows, index):
        there = array.at[pl.ds(0, rows), :]
        remote(there, there, sends.at[index], small_recv.at[0], {"seq": z}).wait_send()

    peers = (n - 1) * tokens * HD // features
    all_sent(w_ring, 4 * peers, 0)
    pair.wait_send()
    all_gates().wait_send()
    all_sent(w_ring, (n - 1) * share, 3)
    all_sent(other_partial, per_half * share, 4)
    all_sent(att, (MEMBERS - 1) * tokens, 5)
    all_sent(result, others, 6)
    with jax.named_scope("out"):
        there = out.at[pl.ds(0, others), :]
        remote(there, there, sends.at[6], out_recv.at[0], {"seq": z}).wait_recv()


def shards(n, groups, subs, q, k, v, weight, q_gain, k_gain, gate, count):
    tokens, features = q.shape
    width = weight.shape[1]
    share, per_half = width // MEMBERS, n // subs
    hbm = pl.BlockSpec(memory_space=pl.ANY)
    dma = pltpu.SemaphoreType.DMA
    rows = n * tokens
    return pl.pallas_call(
        functools.partial(kernel, n, math.isqrt(groups), subs),
        out_shape=jax.ShapeDtypeStruct((per_half * width, tokens), BF16),
        in_specs=[hbm] * 7 + [pl.BlockSpec(memory_space=pltpu.SMEM)],
        out_specs=pl.BlockSpec(memory_space=pltpu.VMEM),
        scratch_shapes=[
            pltpu.VMEM((tokens, features), BF16),
            pltpu.VMEM((tokens, features), BF16),
            pltpu.VMEM((tokens, features), BF16),
            pltpu.VMEM((1, features), F32),
            pltpu.VMEM((1, features), F32),
            pltpu.VMEM((per_half * width,), F32),
            pltpu.VMEM((per_half * width, HD), F32),
            pltpu.VMEM((2, tokens, HD), F32),
            pltpu.VMEM((2, tokens, HD), F32),
            pltpu.VMEM((n, tokens, HD), BF16),
            pltpu.VMEM((n, tokens, HD), BF16),
            pltpu.VMEM((rows, HD), BF16),
            pltpu.VMEM((rows, HD), BF16),
            pltpu.VMEM((rows, HD), BF16),
            pltpu.VMEM((8, rows), F32),
            pltpu.VMEM((n, tokens, HD), BF16),
            pltpu.VMEM((MEMBERS * tokens, features), BF16),
            pltpu.VMEM((n * share, features), BF16),
            pltpu.VMEM((2, per_half * share, MEMBERS * tokens), F32),
            pltpu.VMEM((per_half * share, MEMBERS * tokens), F32),
            pltpu.VMEM((MEMBERS * per_half * share, HD), F32),
            pltpu.VMEM((MEMBERS * per_half * share, tokens), BF16),
            pltpu.SemaphoreType.REGULAR((1,)),
            pltpu.SemaphoreType.REGULAR((1,)),
            dma((7,)),
            dma((7,)),
            dma((1,)),
            dma((1,)),
            dma((n,)),
            dma((n,)),
            dma((4, n // 2)),
            dma((1,)),
            dma((1,)),
            dma((MEMBERS,)),
            dma((per_half,)),
            dma((1,)),
        ],
        compiler_params=pltpu.CompilerParams(
            collective_id=0, has_side_effects=True, vmem_limit_bytes=40 * 2**20
        ),
        name="attention",
    )(*(pltpu.with_memory_space_constraint(x, pltpu.HBM) for x in (q, k, v, weight.T, q_gain.reshape(1, -1), k_gain.reshape(1, -1), gate)), count).T


def solution(mesh):
    placed = (
        P(("groups", "seq"), "sub"),
        P(("groups", "seq"), "sub"),
        P(("groups", "seq"), "sub"),
        P("sub", "seq"),
        P("sub"),
        P("sub"),
        P(("groups", "sub")),
        P("groups"),
    )
    return jax.shard_map(
        functools.partial(shards, mesh.shape["seq"], mesh.shape["groups"], mesh.shape["sub"]),
        mesh=mesh,
        in_specs=placed,
        out_specs=P(("groups", "seq"), "sub"),
        check_vma=False,
    )
```

```python
import functools
import math

import jax
import jax.numpy as jnp
from jax import lax
from jax.experimental import pallas as pl
from jax.experimental.pallas import tpu as pltpu
from jax.sharding import PartitionSpec as P

HD = 128
EPSILON = 1e-06
MEMBERS = 4
CUTS = (48, 32)
IN_ATTENTION = ((1, 0),)
IN_RETURN = ((6, 1),)
IN_SQUARE = {1: 2}
IN_PROJECTION = ((5, 3), (7, 4), (9, 5), (11, 6), (13, 7))
F32, BF16 = jnp.float32, jnp.bfloat16


def remote(source, target, send, arrive, where):
    return pltpu.make_async_remote_copy(
        src_ref=source,
        dst_ref=target,
        send_sem=send,
        recv_sem=arrive,
        device_id=where,
        device_id_type=pl.DeviceIdType.MESH,
    )


def nt(left, right):
    return lax.dot_general(left, right, (((1,), (1,)), ((), ())), preferred_element_type=F32)


def kernel(
    n, side, subs,
    q_any, k_any, v_any, w_any, q_gain_any, k_gain_any, gate_any, count,
    out,
    q_in, k_in, v_in, q_gain, k_gain, gate_in, gate_turned, squares, squares_in, kn, qn, k_all, v_all, q_all, bias, o_out,
    att, w_ring, partial, other_partial, gates, result,
    from_up, from_down, load, sends, v_recv, k_recv, q_recv, o_recv,
    ring_recv, small_recv, gate_recv, att_recv, pair_recv, out_recv,
):
    tokens, features = q_in.shape
    share = w_any.shape[0] // MEMBERS
    per_half = n // subs
    z = lax.axis_index("seq")
    s = lax.axis_index("sub")
    g = lax.axis_index("groups")
    gx, gy = g % side, g // side
    bx, by = gx % 2, gy % 2
    me = 2 * by + bx

    def square(e):
        there = g + (e % 2) * (1 - 2 * bx) + (e // 2) * side * (1 - 2 * by)
        return there, 2 * ((by + e // 2) % 2) + (bx + e) % 2

    def hop(i):
        return (i % 2) * ((i + 1) // 2) + (1 - i % 2) * ((n - i // 2) % n)

    def far(i):
        return hop((n - i) % n)

    barrier = pltpu.get_barrier_semaphore()

    near = n // 8

    def greet(i, carry):
        pl.semaphore_signal(barrier, inc=1, device_id={"seq": (z + far(i)) % n}, device_id_type=pl.DeviceIdType.MESH)
        return carry

    lax.fori_loop(n - 2 * near, n, greet, 0)
    pl.semaphore_signal(barrier, inc=1, device_id={"sub": 1 - s}, device_id_type=pl.DeviceIdType.MESH)
    for e in range(1, MEMBERS):
        pl.semaphore_signal(barrier, inc=1, device_id={"groups": square(e)[0]}, device_id_type=pl.DeviceIdType.MESH)

    loads = [
        pltpu.make_async_copy(source, target, load.at[index])
        for index, (source, target) in enumerate((
            (v_any, v_in), (k_any, k_in), (q_any, q_in), (k_gain_any, k_gain), (q_gain_any, q_gain), (gate_any, gate_in),
        ))
    ]
    for copy in loads:
        copy.start()

    weight_load = pltpu.make_async_copy(
        w_any.at[pl.ds(pl.multiple_of(me * share, 16), share), :],
        w_ring.at[pl.ds(pl.multiple_of(z * share, 16), share), :],
        load.at[6],
    )
    weight_load.start()

    def ring(k, upwards, chunk):
        plane = (z - k + n) % n if upwards else (z + k) % n
        start = plane * share + sum(CUTS[:chunk])
        rows = w_ring.at[pl.ds(pl.multiple_of(start, 16), CUTS[chunk]), :]
        to = (z + 1) % n if upwards else (z + n - 1) % n
        lane = 2 * chunk + upwards
        return remote(rows, rows, sends.at[3], ring_recv.at[lane, k], {"seq": to})

    ways = [(upwards, chunk, n // 2 - (upwards != (chunk == 0))) for chunk in (0, 1) for upwards in (True, False)]

    def relay(k):
        if k:
            with jax.named_scope(f"relay{k}"):
                for upwards, chunk, hops in ways:
                    if k <= hops:
                        ring_arrival(k, upwards, chunk).wait_recv()
                    if k < hops:
                        ring(k, upwards, chunk).start()
        else:
            for upwards, chunk, hops in ways:
                ring(0, upwards, chunk).start()

    def ring_arrival(k, upwards, chunk):
        plane = (z - k + n) % n if upwards else (z + k) % n
        start = plane * share + sum(CUTS[:chunk])
        rows = w_ring.at[pl.ds(pl.multiple_of(start, 16), CUTS[chunk]), :]
        lane = 2 * chunk + upwards
        return remote(rows, rows, sends.at[3], ring_recv.at[lane, k - 1], {"seq": z})

    loads[0].wait()
    with jax.named_scope("barrier"):
        pl.semaphore_wait(barrier, 2 * near + 1 + MEMBERS - 1)

    own = pl.ds(pl.multiple_of(z * tokens, tokens), tokens)

    def v_block(there):
        return v_in.at[:, pl.ds(pl.multiple_of(there * HD, HD), HD)]

    exchanges = (
        (v_block, v_all, lambda d: v_recv.at[0]),
        (lambda there: kn.at[there], k_all, lambda d: k_recv.at[0]),
        (lambda there: qn.at[there], q_all, lambda d: q_recv.at[d]),
    )

    def to_peers(array, first, last):
        source, target, arrive = exchanges[array]

        def one(i, carry):
            d = hop(i)
            there = (z + d) % n
            remote(source(there), target.at[own, :], sends.at[0], arrive(d), {"seq": there}).start()
            return carry

        lax.fori_loop(first, last, one, 0)

    weight_load.wait()
    for known in range(near, n // 2, near):
        pl.semaphore_signal(from_down.at[0], inc=1, device_id={"seq": (z + near) % n}, device_id_type=pl.DeviceIdType.MESH)
        pl.semaphore_signal(from_up.at[0], inc=1, device_id={"seq": (z + n - near) % n}, device_id_type=pl.DeviceIdType.MESH)
        to_peers(0, 1 + 2 * (known - near), 1 + 2 * known)
        with jax.named_scope("beyond"):
            pl.semaphore_wait(from_down.at[0], 1)
            pl.semaphore_wait(from_up.at[0], 1)
    to_peers(0, 1 + 2 * (n // 2 - near), n)

    for index, array in enumerate((k_in, q_in)):
        loads[1 + index].wait()
        total = jnp.zeros((tokens, HD), F32)
        for head in range(features // HD):
            wide = array[:, head * HD : (head + 1) * HD].astype(F32)
            total = total + wide * wide
        squares[index] = total

    pair = remote(squares, squares_in, sends.at[1], small_recv.at[0], {"sub": 1 - s})
    pair.start()

    loads[5].wait()
    gate = gate_in[...].reshape(1, gate_in.shape[0])
    for first in range(0, gate_in.shape[0], HD):
        gate_turned[first : first + HD, :] = jnp.transpose(jnp.broadcast_to(gate[:, first : first + HD], (HD, HD)))
    def gate_rows(i, number):
        return pl.ds(pl.multiple_of((i * MEMBERS + number) * share, 16), share)

    def gate_copy(i, e):
        there, number = square(e)
        return remote(gate_turned.at[gate_rows(i, number), :],
                      gates.at[pl.ds(pl.multiple_of((me * per_half + i) * share, 16), share), :],
                      sends.at[2], gate_recv.at[0], {"groups": there})

    def gate_out(i, carry):
        for e in range(1, MEMBERS):
            gate_copy(i, e).start()
        gates[pl.ds(pl.multiple_of((me * per_half + i) * share, 16), share), :] = gate_turned[gate_rows(i, me), :]
        return carry

    lax.fori_loop(0, per_half, gate_out, 0)

    pair.wait_recv()
    loads[3].wait()
    loads[4].wait()
    for index, (array, gain, normed, full) in enumerate(((k_in, k_gain, kn, k_all), (q_in, q_gain, qn, q_all))):
        total = jnp.sum(squares[index] + squares_in[index], axis=1, keepdims=True)
        inverse = lax.rsqrt(total / (features * subs) + EPSILON)
        for head in range(features // HD):
            here = slice(head * HD, (head + 1) * HD)
            normed[head] = (array[:, here].astype(F32) * inverse * gain[:, here]).astype(BF16)
        to_peers(1 + index, 1, n)
        full[own, :] = normed[z]
    v_all[own, :] = v_in[:, pl.ds(pl.multiple_of(z * HD, HD), HD)]
    positions = lax.broadcasted_iota(jnp.int32, bias.shape, 1)
    bias[...] = jnp.where(positions < count[0], 0.0, -1e30)

    def whole(array, arrive):
        there = array.at[pl.ds(0, (n - 1) * tokens), :]
        return remote(there, there, sends.at[0], arrive.at[0], {"seq": z})

    with jax.named_scope("vk"):
        whole(v_all, v_recv).wait_recv()
        whole(k_all, k_recv).wait_recv()
    factor = math.log2(math.e) / math.sqrt(HD)
    mine = pl.ds(pl.multiple_of(me * tokens, tokens), tokens)

    def o_copy(d):
        lanes = pl.ds(pl.multiple_of(z * HD, HD), HD)
        return remote(o_out.at[d], att.at[mine, lanes], sends.at[0], o_recv.at[d], {"seq": (z - d + n) % n})

    def attend(i, carry):
        d = hop(i)
        rows = pl.ds(pl.multiple_of(((z - d + n) % n) * tokens, tokens), tokens)

        @pl.when(i > 0)
        def _():
            there = q_all.at[own, :]
            with jax.named_scope("q"):
                remote(there, there, sends.at[0], q_recv.at[d], {"seq": z}).wait_recv()

        scores = nt(q_all[rows, :], k_all[...]) * factor + bias[0:1, :]
        weights = jnp.exp2(scores - jnp.max(scores, axis=1, keepdims=True))
        denominator = jnp.sum(weights, axis=1, keepdims=True)
        summed = jnp.dot(weights.astype(BF16), v_all[...], preferred_element_type=F32)
        o_out[d] = (summed / denominator).astype(BF16)

        @pl.when(i > 0)
        def _():
            o_copy(d).start()

        return carry

    def spread(body, first, last, points):
        for stop, k in points:
            lax.fori_loop(first, stop, body, 0)
            relay(k)
            first = stop
        lax.fori_loop(first, last, body, 0)

    with jax.named_scope("attend"):
        spread(attend, 0, n, IN_ATTENTION)
    att[mine, pl.ds(pl.multiple_of(z * HD, HD), HD)] = o_out[0]

    def square_copy(d, e):
        lanes = pl.ds(pl.multiple_of(((z + d) % n) * HD, HD), HD)
        return remote(att.at[mine, lanes], att.at[mine, lanes], sends.at[5], att_recv.at[e], {"groups": square(e)[0]})

    def o_arrived(i, carry):
        d = hop(i)

        @pl.when(i > 0)
        def _():
            o_copy(d).wait_recv()

        for e in range(1, MEMBERS):
            square_copy(d, e).start()
        return carry

    with jax.named_scope("o"):
        spread(o_arrived, 0, n, IN_RETURN)

    for e in range(1, MEMBERS):
        rows = att.at[pl.ds(pl.multiple_of(square(e)[1] * tokens, tokens), tokens), :]
        with jax.named_scope(f"square{e}"):
            remote(rows, rows, sends.at[5], att_recv.at[e], {"sub": s}).wait_recv()
        if e in IN_SQUARE:
            relay(IN_SQUARE[e])
    others = (MEMBERS - 1) * per_half * share

    def all_gates():
        there = gates.at[pl.ds(0, others), :]
        return remote(there, there, sends.at[2], gate_recv.at[0], {"seq": z})

    all_gates().wait_recv()

    def place(i):
        return pl.ds(pl.multiple_of(i * share, 16), share)

    def give(i):
        return remote(partial.at[1, place(i), :], other_partial.at[place(i), :],
                      sends.at[4], pair_recv.at[i], {"sub": 1 - s})

    def out_copy(i, e):
        there, number = square(e)
        return remote(result.at[pl.ds(pl.multiple_of((number * per_half + i) * share, 16), share), :],
                      out.at[gate_rows(i, me), :], sends.at[6], out_recv.at[0], {"groups": there})

    def project(j, carry):
        plane = (z + hop(j)) % n
        i = plane % per_half
        mine = plane // per_half == s
        with jax.named_scope("project"):
            total = nt(w_ring[pl.ds(pl.multiple_of(plane * share, 16), share), :], att[...])
            partial[jnp.where(mine, 0, 1), place(i), :] = total

        @pl.when(jnp.logical_not(mine))
        def _():
            give(i).start()

        @pl.when((j >= 2) & (j < n - 1))
        def _():
            finish(j - 2)

        return carry

    def finish(j):
        plane = (z + hop(j)) % n
        i = plane % per_half

        @pl.when(plane // per_half == s)
        def _():
            with jax.named_scope("pair"):
                give(i).wait_recv()
            for number in range(MEMBERS):
                rows = pl.ds(pl.multiple_of((number * per_half + i) * share, 16), share)
                lanes = slice(number * tokens, (number + 1) * tokens)
                total = partial[0, place(i), lanes] + other_partial[place(i), lanes]
                result[rows, :] = (total * gates[rows, :]).astype(BF16)
            for e in range(1, MEMBERS):
                out_copy(i, e).start()
            out[gate_rows(i, me), :] = result[pl.ds(pl.multiple_of((me * per_half + i) * share, 16), share), :]

    spread(project, 0, n - 1, IN_PROJECTION)
    relay(n // 2)
    project(n - 1, 0)
    for j in (3, 2, 1):
        finish(n - j)

    def all_sent(array, rows, index):
        there = array.at[pl.ds(0, rows), :]
        remote(there, there, sends.at[index], small_recv.at[0], {"seq": z}).wait_send()

    peers = (n - 1) * tokens * HD // features
    all_sent(w_ring, 4 * peers, 0)
    pair.wait_send()
    all_gates().wait_send()
    all_sent(w_ring, (n - 1) * share, 3)
    all_sent(other_partial, per_half * share, 4)
    all_sent(att, (MEMBERS - 1) * tokens, 5)
    all_sent(result, others, 6)
    with jax.named_scope("out"):
        there = out.at[pl.ds(0, others), :]
        remote(there, there, sends.at[6], out_recv.at[0], {"seq": z}).wait_recv()


def shards(n, groups, subs, q, k, v, weight, q_gain, k_gain, gate, count):
    tokens, features = q.shape
    width = weight.shape[1]
    share, per_half = width // MEMBERS, n // subs
    hbm = pl.BlockSpec(memory_space=pl.ANY)
    dma = pltpu.SemaphoreType.DMA
    rows = n * tokens
    return pl.pallas_call(
        functools.partial(kernel, n, math.isqrt(groups), subs),
        out_shape=jax.ShapeDtypeStruct((per_half * width, tokens), BF16),
        in_specs=[hbm] * 7 + [pl.BlockSpec(memory_space=pltpu.SMEM)],
        out_specs=pl.BlockSpec(memory_space=pltpu.VMEM),
        scratch_shapes=[
            pltpu.VMEM((tokens, features), BF16),
            pltpu.VMEM((tokens, features), BF16),
            pltpu.VMEM((tokens, features), BF16),
            pltpu.VMEM((1, features), F32),
            pltpu.VMEM((1, features), F32),
            pltpu.VMEM((per_half * width,), F32),
            pltpu.VMEM((per_half * width, HD), F32),
            pltpu.VMEM((2, tokens, HD), F32),
            pltpu.VMEM((2, tokens, HD), F32),
            pltpu.VMEM((n, tokens, HD), BF16),
            pltpu.VMEM((n, tokens, HD), BF16),
            pltpu.VMEM((rows, HD), BF16),
            pltpu.VMEM((rows, HD), BF16),
            pltpu.VMEM((rows, HD), BF16),
            pltpu.VMEM((8, rows), F32),
            pltpu.VMEM((n, tokens, HD), BF16),
            pltpu.VMEM((MEMBERS * tokens, features), BF16),
            pltpu.VMEM((n * share, features), BF16),
            pltpu.VMEM((2, per_half * share, MEMBERS * tokens), F32),
            pltpu.VMEM((per_half * share, MEMBERS * tokens), F32),
            pltpu.VMEM((MEMBERS * per_half * share, HD), F32),
            pltpu.VMEM((MEMBERS * per_half * share, tokens), BF16),
            pltpu.SemaphoreType.REGULAR((1,)),
            pltpu.SemaphoreType.REGULAR((1,)),
            dma((7,)),
            dma((7,)),
            dma((1,)),
            dma((1,)),
            dma((n,)),
            dma((n,)),
            dma((4, n // 2)),
            dma((1,)),
            dma((1,)),
            dma((MEMBERS,)),
            dma((per_half,)),
            dma((1,)),
        ],
        compiler_params=pltpu.CompilerParams(
            collective_id=0, has_side_effects=True, vmem_limit_bytes=40 * 2**20
        ),
        name="attention",
    )(*(pltpu.with_memory_space_constraint(x, pltpu.HBM) for x in (q, k, v, weight.T, q_gain.reshape(1, -1), k_gain.reshape(1, -1), gate)), count).T


def solution(mesh):
    placed = (
        P(("groups", "seq"), "sub"),
        P(("groups", "seq"), "sub"),
        P(("groups", "seq"), "sub"),
        P("sub", "seq"),
        P("sub"),
        P("sub"),
        P(("groups", "sub")),
        P("groups"),
    )
    return jax.shard_map(
        functools.partial(shards, mesh.shape["seq"], mesh.shape["groups"], mesh.shape["sub"]),
        mesh=mesh,
        in_specs=placed,
        out_specs=P(("groups", "seq"), "sub"),
        check_vma=False,
    )
```
